32 devices in a mesh: row: 4 (over y, x), col: 8 (over z, core).
Axes of the slice: x: 2, y: 2, z: 4, core: 2. Of those that a mesh axis runs over, the one named last changes fastest.
Arguments:
- values: bfloat16 [4096, 4096], P('row', 'col'), may hold values from 0.0001296997 to 0.12988281
- tile_mask: int32 [32, 32], P('row', 'col'), may hold values 0 or 1
- keep_mask: int32 [32, 32], P('row', 'col'), may hold values 0 or 1
- thr_index: int32 [4096], P('col'), may hold values from 0 to 9
Outputs:
- expanded: bfloat16 [4096, 4096], P('row', 'col')
The draws below stay inside these ranges and needn't reach their ends.
All inputs are finite; a program needn't handle non-finite values. No bound on the sum of `tile_mask` or of `keep_mask` on one device may be relied on, other than what follows from the above.
Results may differ from the reference program's by a relative error of at most 0.0004.
Values may be sent and summed in bfloat16 or wider, within the bound.
No kernel may reach another device: no remote copies, remote signals or barrier semaphores. Data moves between devices by JAX's collectives and lax.ppermute only.
A program may use at most 64 MiB of HBM per device.

```python
import math
import jax
import jax.numpy as jnp

TB = 128
NT = 32
ORDER = 4096


def touch_ends(values, stream_key, smallest, largest):
    spot = [jax.random.randint(jax.random.fold_in(stream_key, axis), (), 0, length) for axis, length in enumerate(values.shape)]
    longest = values.shape.index(max(values.shape))
    neighbour = spot[:longest] + [(spot[longest] + 1) % values.shape[longest]] + spot[longest + 1:]
    return values.at[tuple(spot)].set(smallest).at[tuple(neighbour)].set(largest)


def levels(stream_key, extent, shards, least, largest):
    level = 1.0
    for dim, shards_of in shards:
        draws = jax.random.uniform(jax.random.fold_in(jax.random.fold_in(stream_key, 6), dim), (shards_of,), jnp.float32, least / len(shards), largest / len(shards))
        level = level * jnp.repeat(jnp.exp(draws), extent[dim] // shards_of).reshape((-1,) + (1,) * (len(extent) - 1 - dim))
    return level


def setup_inputs(seed: int = 0) -> dict:
    seeds = jax.random.split(jax.random.key(seed), 5)
    values = jnp.clip(jnp.exp(math.log(0.12988281) - 6.909166 * jax.random.uniform(seeds[0], (ORDER, ORDER), jnp.float32) ** levels(seeds[0], (ORDER, ORDER), ((0, 4), (1, 8)), -0.2, 0.2)), 0.0001296997, 0.12988281).astype(jnp.bfloat16)
    tile_mask = touch_ends((jax.random.randint(seeds[1], (NT, NT), 0, 2) < 1).astype(jnp.int32), jax.random.fold_in(seeds[1], 1), 0, 1)
    keep_mask = touch_ends((jax.random.randint(seeds[2], (NT, NT), 0, 4) < 3).astype(jnp.int32), jax.random.fold_in(seeds[2], 1), 0, 1)
    thr_index = touch_ends(jax.random.randint(seeds[3], (ORDER,), 0, 10), jax.random.fold_in(seeds[3], 1), 0, 9).astype(jnp.int32)
    return {"values": values, "tile_mask": tile_mask, "keep_mask": keep_mask, "thr_index": thr_index}


def reference(values, tile_mask, keep_mask, thr_index):
    matrix = (values.reshape(NT, TB, NT, TB) * tile_mask[:, None, :, None].astype(jnp.bfloat16)).reshape(ORDER, ORDER)
    product = jnp.dot(matrix, matrix, preferred_element_type=jnp.float32)
    col_means = jnp.sum(product, axis=0) / ORDER
    thresholds = 0.125 * thr_index.astype(jnp.float32)
    kept_cells = jnp.broadcast_to(keep_mask[:, None, :, None].astype(jnp.float32), (NT, TB, NT, TB)).reshape(ORDER, ORDER)
    pruned = jnp.maximum(product - thresholds * col_means, 0.0) * kept_cells
    col_totals = jnp.sum(pruned, axis=0) / ORDER
    return (pruned / jnp.maximum(col_totals, 0.1)).astype(jnp.bfloat16)
```

```python
import functools

import jax
import jax.numpy as jnp
from jax import lax
from jax.experimental import pallas as pl
from jax.experimental.pallas import tpu as pltpu
from jax.sharding import PartitionSpec as P

TB = 128
PAD = 16
AXES = ("row", "col")
F32, BF16, I32 = jnp.float32, jnp.bfloat16, jnp.int32
ANY = pl.BlockSpec(memory_space=pl.ANY)
VMEM = pl.BlockSpec(memory_space=pltpu.VMEM)
SMEM = pl.BlockSpec(memory_space=pltpu.SMEM)


def params(limit=56):
    return pltpu.CompilerParams(vmem_limit_bytes=limit * 1024 * 1024)


def cost(flops, moved):
    return pl.CostEstimate(flops=int(flops), bytes_accessed=int(moved), transcendentals=0)


def tiles_of(shape):
    return shape[0] // TB, shape[1] // TB


def pack_kernel(slots, mask_ref, block_ref, out_ref):
    ti, tj = tiles_of(block_ref.shape)
    lane = lax.broadcasted_iota(I32, (PAD, TB), 1)
    table = jnp.full((PAD, TB), -1, I32)
    used = jnp.int32(0)
    for i in range(ti):
        for j in range(tj):
            stored = mask_ref[j, i]
            fits = jnp.logical_and(stored > 0, used < slots)

            @pl.when(fits)
            def _(i=i, j=j, used=used):
                at = pl.multiple_of(used * TB, TB)
                out_ref[pl.ds(at, TB), :] = block_ref[i * TB : (i + 1) * TB, j * TB : (j + 1) * TB]

            table = jnp.where(lane == i * tj + j, jnp.where(fits, used, -1), table)
            used = used + stored
    table = jnp.where(lane == ti * tj, used, table)
    out_ref[slots * TB :, :] = table.astype(F32).astype(BF16)


def pack(block, mask_t, slots):
    return pl.pallas_call(
        functools.partial(pack_kernel, slots),
        out_shape=jax.ShapeDtypeStruct((slots * TB + PAD, TB), BF16),
        in_specs=[SMEM, VMEM],
        out_specs=VMEM,
        compiler_params=params(),
        cost_estimate=cost(1e6, 2 * block.size * 2),
        name="pack",
    )(mask_t, block)


def read_table(slots, buf, at, itab, stab, sem):
    itab[...] = buf[slots * TB : slots * TB + 8, :].astype(F32).astype(I32)
    copy = pltpu.make_async_copy(itab, stab.at[at], sem)
    copy.start()
    copy.wait()


def tile_from(buf, slot):
    at = pl.multiple_of(jnp.maximum(slot, 0) * TB, TB)
    return jnp.where(slot >= 0, buf[pl.ds(at, TB), :], jnp.zeros((TB, TB), BF16))


def panel_kernel(slots, n, rows, me_ref, *refs):
    bufs, (panel_ref, sums_ref), (itab, stab, sem) = refs[:n], refs[n : n + 2], refs[n + 2 :]
    cols = panel_ref.shape[1]
    ti, tj = rows // TB, cols // TB
    worst = jnp.int32(0)
    sums_ref[...] = jnp.zeros_like(sums_ref)
    for q in range(n):
        read_table(slots, bufs[q], q, itab, stab, sem)
        worst = jnp.maximum(worst, stab[q, 0, ti * tj])
        base = (me_ref[0] ^ q) * rows

        @pl.loop(0, ti)
        def _(i, q=q, base=base):
            for j in range(tj):
                tile = tile_from(bufs[q], stab[q, 0, i * tj + j])
                panel_ref[pl.ds(pl.multiple_of(base + i * TB, TB), TB), j * TB : (j + 1) * TB] = tile
                part = jnp.sum(tile.astype(F32), axis=0, keepdims=True)
                sums_ref[j : j + 1, :] += part

    flag = jnp.where(worst > slots, 1.0, 0.0)
    sums_ref[tj : tj + 1, :] = jnp.full((1, TB), 1.0, F32) * flag


def panel(me, payloads, slots, rows, cols):
    n = len(payloads)
    s_rows = -(-(cols // TB + 1) // 8) * 8
    return pl.pallas_call(
        functools.partial(panel_kernel, slots, n, rows),
        out_shape=(
            jax.ShapeDtypeStruct((n * rows, cols), BF16),
            jax.ShapeDtypeStruct((s_rows, TB), F32),
        ),
        in_specs=[SMEM] + [VMEM] * n,
        out_specs=(VMEM, VMEM),
        scratch_shapes=[
            pltpu.VMEM((8, TB), I32),
            pltpu.SMEM((n, 8, TB), I32),
            pltpu.SemaphoreType.DMA,
        ],
        compiler_params=params(),
        cost_estimate=cost(1e7, 2 * n * rows * cols * 2),
        name="panel",
    )(me, *payloads)


def unpack_row(slots, buf, at, rows, cols, itab, stab, sem, lhs, lane0):
    ti, tj = rows // TB, cols // TB
    read_table(slots, buf, at, itab, stab, sem)

    @pl.loop(0, ti)
    def _(i):
        for j in range(tj):
            tile = tile_from(buf, stab[at, 0, i * tj + j])
            lhs[pl.ds(pl.multiple_of(i * TB, TB), TB), pl.ds(pl.multiple_of(lane0 + j * TB, TB), TB)] = tile


def row_step(rows):
    return min(rows, 256)


def dot_kernel(slots, pairs, rows, cols, me_ref, *refs):
    n = 2 * pairs
    bufs, panel_ref, acc_ref = refs[:n], refs[n], refs[n + 1]
    itab, stab, sem, lhs = refs[n + 2 :]
    core, z = me_ref[1], me_ref[2]
    step = row_step(rows)
    for q in range(pairs):
        unpack_row(slots, bufs[2 * q], 2 * q, rows, cols, itab, stab, sem, lhs, core * cols)
        unpack_row(slots, bufs[2 * q + 1], 2 * q + 1, rows, cols, itab, stab, sem, lhs, (1 - core) * cols)
        at = pl.multiple_of((z ^ q) * 2 * cols, TB)

        @pl.loop(0, rows // step)
        def _(m, q=q, at=at):
            here = pl.ds(pl.multiple_of(m * step, step), step)
            got = jnp.dot(lhs[here, :], panel_ref[pl.ds(at, 2 * cols), :], preferred_element_type=F32)
            acc_ref[here, :] = got if q == 0 else acc_ref[here, :] + got


def dots(me, payloads, dense, slots, rows, cols):
    pairs = len(payloads) // 2
    return pl.pallas_call(
        functools.partial(dot_kernel, slots, pairs, rows, cols),
        out_shape=jax.ShapeDtypeStruct((rows, cols), F32),
        in_specs=[SMEM] + [VMEM] * (2 * pairs + 1),
        out_specs=VMEM,
        scratch_shapes=[
            pltpu.VMEM((8, TB), I32),
            pltpu.SMEM((2 * pairs, 8, TB), I32),
            pltpu.SemaphoreType.DMA,
            pltpu.VMEM((rows, 2 * cols), BF16),
        ],
        compiler_params=params(),
        cost_estimate=cost(2 * rows * 2 * cols * pairs * cols, 12 * rows * cols * pairs),
        name="dots",
    )(me, *payloads, dense)


def means_kernel(n_pairs, s_rows, order, me_ref, *refs):
    msgs, thr_ref, panel_ref, out_ref = refs[:n_pairs], *refs[n_pairs:]
    core, z = me_ref[1], me_ref[2]
    cols = panel_ref.shape[1]
    tj = cols // TB
    total = jnp.zeros((8, cols), F32)
    row = lax.broadcasted_iota(I32, (8, TB), 0)
    for q in range(n_pairs):
        for b in range(2):
            for t in range(tj):
                s = jnp.broadcast_to(msgs[q][b * s_rows + t : b * s_rows + t + 1, :], (8, TB))
                high = s.astype(BF16).astype(F32)
                mid = (s - high).astype(BF16).astype(F32)
                low = s - high - mid
                lhs = jnp.where(row == 0, high, jnp.where(row == 1, mid, jnp.where(row == 2, low, 0.0)))
                at = (z ^ q) * 2 * cols + (core ^ b) * cols + t * TB
                total += jnp.dot(
                    lhs.astype(BF16),
                    panel_ref[pl.ds(pl.multiple_of(at, TB), TB), :],
                    preferred_element_type=F32,
                )
    mean = jnp.sum(total, axis=0, keepdims=True) / order
    out_ref[...] = jnp.broadcast_to(0.125 * thr_ref[...].astype(F32) * mean, out_ref.shape)


def cuts_of(me, messages, thr, dense, s_rows, order):
    n = len(messages)
    cols = dense.shape[1]
    return pl.pallas_call(
        functools.partial(means_kernel, n, s_rows, order),
        out_shape=jax.ShapeDtypeStruct((8, cols), F32),
        in_specs=[SMEM] + [VMEM] * (n + 2),
        out_specs=VMEM,
        compiler_params=params(),
        cost_estimate=cost(1e7, dense.size * 2),
        name="cuts",
    )(me, *messages, thr, dense)


def last_kernel(slots, n_parts, pair, rows, cols, me_ref, keep_ref, *refs):
    parts = refs[: 2 * n_parts]
    panel_ref, prior_ref, cut_ref, acc_ref, tot_ref = refs[2 * n_parts : 2 * n_parts + 5]
    mine, other, itab, stab, sem, lhs, rhs, sems = refs[2 * n_parts + 5 :]
    core, z, part = me_ref[1], me_ref[2], me_ref[3]
    step = row_step(rows)
    at = pl.multiple_of((z ^ pair) * 2 * cols, TB)
    get = pltpu.make_async_copy(panel_ref.at[pl.ds(at, 2 * cols), :], rhs, sems.at[2])
    get.start()
    for p in range(n_parts):

        @pl.when(part == p)
        def _(p=p):
            pltpu.make_async_copy(parts[2 * p], mine, sems.at[0]).start()
            pltpu.make_async_copy(parts[2 * p + 1], other, sems.at[1]).start()

    pltpu.make_async_copy(parts[0], mine, sems.at[0]).wait()
    unpack_row(slots, mine, 0, rows, cols, itab, stab, sem, lhs, core * cols)
    pltpu.make_async_copy(parts[1], other, sems.at[1]).wait()
    unpack_row(slots, other, 1, rows, cols, itab, stab, sem, lhs, (1 - core) * cols)
    get.wait()
    tot_ref[...] = jnp.zeros_like(tot_ref)
    cut = cut_ref[0:1, :]
    per = step // TB

    @pl.loop(0, rows // step)
    def _(m):
        here = pl.ds(pl.multiple_of(m * step, step), step)
        got = prior_ref[here, :] + jnp.dot(lhs[here, :], rhs[...], preferred_element_type=F32)
        got = jnp.maximum(got - cut, 0.0)
        for a in range(per):
            for j in range(cols // TB):
                kept = keep_ref[j, m * per + a].astype(F32)
                cell = got[a * TB : (a + 1) * TB, j * TB : (j + 1) * TB] * kept
                acc_ref[pl.ds(pl.multiple_of(m * step + a * TB, TB), TB), j * TB : (j + 1) * TB] = cell
                tot_ref[:, j * TB : (j + 1) * TB] += jnp.sum(cell.reshape(TB // 8, 8, TB), axis=0)


def finish(me, keep_t, parts, dense, prior, cut, slots, pair, rows, cols):
    n_parts = len(parts) // 2
    return pl.pallas_call(
        functools.partial(last_kernel, slots, n_parts, pair, rows, cols),
        out_shape=(jax.ShapeDtypeStruct((rows, cols), F32), jax.ShapeDtypeStruct((8, cols), F32)),
        in_specs=[SMEM, SMEM] + [ANY] * (2 * n_parts + 1) + [VMEM, VMEM],
        out_specs=(VMEM, VMEM),
        scratch_shapes=[
            pltpu.VMEM(parts[0].shape, BF16),
            pltpu.VMEM(parts[0].shape, BF16),
            pltpu.VMEM((8, TB), I32),
            pltpu.SMEM((2, 8, TB), I32),
            pltpu.SemaphoreType.DMA,
            pltpu.VMEM((rows, 2 * cols), BF16),
            pltpu.VMEM((2 * cols, cols), BF16),
            pltpu.SemaphoreType.DMA((3,)),
        ],
        compiler_params=params(),
        cost_estimate=cost(2 * rows * 2 * cols * cols, 12 * rows * cols),
        name="finish",
    )(me, keep_t, *parts, dense, prior, cut)


def scale_kernel(n, order, x_ref, *refs):
    tots, out_ref = refs[:n], refs[n]
    total = tots[0][...]
    for t in tots[1:]:
        total = total + t[...]
    total = jnp.sum(total, axis=0, keepdims=True) / order
    out_ref[...] = (x_ref[...] / jnp.maximum(total, 0.1)).astype(BF16)


def scale(x, totals, order):
    rows, cols = x.shape
    step = row_step(rows)
    n = len(totals)
    return pl.pallas_call(
        functools.partial(scale_kernel, n, order),
        out_shape=jax.ShapeDtypeStruct(x.shape, BF16),
        grid=(rows // step,),
        in_specs=[pl.BlockSpec((step, cols), lambda i: (i, 0))]
        + [pl.BlockSpec((8, cols), lambda i: (0, 0))] * n,
        out_specs=pl.BlockSpec((step, cols), lambda i: (i, 0)),
        compiler_params=params(),
        cost_estimate=cost(2 * x.size, 6 * x.size),
        name="scale",
    )(x, *totals)


def dense_path(values, tile_mask, keep_mask, thr_index, n_row, n_col):
    rows, cols = values.shape
    ti, tj = tiles_of(values.shape)
    matrix = (
        values.reshape(ti, TB, tj, TB) * tile_mask[:, None, :, None].astype(BF16)
    ).reshape(rows, cols)
    kept = jnp.broadcast_to(keep_mask[:, None, :, None].astype(F32), (ti, TB, tj, TB)).reshape(rows, cols)
    r, c = lax.axis_index("row"), lax.axis_index("col")
    order = rows * n_row

    def col_ring(i, carry):
        block, panel_ = carry
        panel_ = lax.dynamic_update_slice(panel_, block, (((r - i) % n_row) * rows, 0))
        return lax.ppermute(block, "row", [(k, (k + 1) % n_row) for k in range(n_row)]), panel_

    _, panel_ = lax.fori_loop(0, n_row, col_ring, (matrix, jnp.zeros((order, cols), BF16)))

    def row_ring(i, carry):
        block, acc = carry
        part = lax.dynamic_slice(panel_, (((c - i) % n_col) * cols, 0), (cols, cols))
        acc = acc + jnp.dot(block, part, preferred_element_type=F32)
        return lax.ppermute(block, "col", [(k, (k + 1) % n_col) for k in range(n_col)]), acc

    _, product = lax.fori_loop(0, n_col, row_ring, (matrix, jnp.zeros((rows, cols), F32)))
    means = lax.psum(jnp.sum(product, axis=0), "row") / order
    pruned = jnp.maximum(product - 0.125 * thr_index.astype(F32) * means, 0.0) * kept
    totals = lax.psum(jnp.sum(pruned, axis=0), "row") / order
    return (pruned / jnp.maximum(totals, 0.1)).astype(BF16)


def line_plan(n_z):
    plan = {}
    for dist in range(1, n_z):
        for j in range(1, n_z):
            groups = {}
            for z in range(n_z):
                b = z ^ j
                if abs(z - b) != dist:
                    continue
                if dist <= 2:
                    groups.setdefault(("own", None), []).append((b, z))
                else:
                    near = z + (1 if b > z else -1)
                    jn = near ^ b
                    part = next(p for p, g in enumerate(plan[jn]) if near in [t for _, t in g[1]])
                    groups.setdefault((jn, part), []).append((near, z))
            for key, pairs in groups.items():
                plan.setdefault(j, []).append((key, pairs))
    merged = {}
    for j, items in plan.items():
        merged[j] = items
    return merged


def on_device(values, tile_mask, keep_mask, thr_index, n_row, n_col):
    return body(values, tile_mask, keep_mask, thr_index, n_row, n_col)


def body(values, tile_mask, keep_mask, thr_index, n_row, n_col):
    rows, cols = values.shape
    ti, tj = tiles_of(values.shape)
    slots = ti * tj * 3 // 4
    n_z = n_col // 2
    order = rows * n_row
    r, c = lax.axis_index("row"), lax.axis_index("col")

    def at(rr, zz, cc):
        return rr * n_col + zz * 2 + cc

    def along_z(pairs):
        return [(at(rr, a, cc), at(rr, b, cc)) for rr in range(n_row) for a, b in pairs for cc in range(2)]

    def along_row(q):
        return [(at(rr, zz, cc), at(rr ^ q, zz, cc)) for rr in range(n_row) for zz in range(n_z) for cc in range(2)]

    def swap_cores(zs):
        return [(at(rr, zz, cc), at(rr, zz, 1 - cc)) for rr in range(n_row) for zz in zs for cc in range(2)]

    def send(x, pairs):
        return lax.ppermute(x, AXES, pairs)

    own = pack(values, tile_mask.T, slots)

    plan = line_plan(n_z)
    got = {}
    done = set()
    for dist in range(1, n_z):
        for j, items in plan.items():
            for p, (key, pairs) in enumerate(items):
                if abs(pairs[0][0] - (pairs[0][1] ^ j)) == 0 and key[0] == "own" and dist == 1:
                    got[(j, p)] = (send(own, along_z(pairs)), [b for _, b in pairs])
                    done.add((j, p))
    while len(done) < sum(len(v) for v in plan.values()):
        for j, items in plan.items():
            for p, (key, pairs) in enumerate(items):
                if (j, p) not in done and key in done:
                    got[(j, p)] = (send(got[key][0], along_z(pairs)), [b for _, b in pairs])
                    done.add((j, p))

    column = [own] + [send(own, along_row(q)) for q in range(1, n_row)]
    swapped = send(own, swap_cores(range(n_z)))
    pairs = [[own, swapped]]
    for j in range(1, n_z):
        entry = []
        for p in range(len(plan[j])):
            x, zs = got[(j, p)]
            entry += [x, send(x, swap_cores(zs))]
        pairs.append(entry)

    z = c // 2
    core = c % 2
    last = n_z - 1
    part_table = [0] * n_z
    for p, (_, prs) in enumerate(plan[last]):
        for _, b in prs:
            part_table[b] = p
    part = jnp.array(part_table, I32)[z]
    me = jnp.stack([r, core, z, part]).astype(I32)

    dense, sums = panel(me, column, slots, rows, cols)
    s_rows = sums.shape[0]
    early = []
    for j in range(last):
        e = pairs[j]
        if len(e) == 2:
            early += e
        else:
            where = [0] * n_z
            for p, (_, prs) in enumerate(plan[j]):
                for _, b in prs:
                    where[b] = p
            pick = jnp.array(where, I32)[z]
            for side in range(2):
                x = e[side]
                for p in range(1, len(e) // 2):
                    x = jnp.where(pick == p, e[2 * p + side], x)
                early.append(x)
    prior = dots(me, early, dense, slots, rows, cols)
    both = jnp.concatenate([sums, send(sums, swap_cores(range(n_z)))], axis=0)
    messages = [both] + [send(both, along_z([(a, a ^ j) for a in range(n_z)])) for j in range(1, n_z)]
    cut = cuts_of(me, messages, thr_index.reshape(1, cols), dense, s_rows, order)
    over = functools.reduce(jnp.maximum, [m[b * s_rows + tj, 0] for m in messages for b in range(2)]) > 0.0

    def fast():
        pruned, tot = finish(
            me, keep_mask.T, pairs[last], dense, prior, cut, slots, last, rows, cols
        )
        totals = [tot] + [send(tot, along_row(q)) for q in range(1, n_row)]
        return scale(pruned, totals, order)

    def full():
        return dense_path(values, tile_mask, keep_mask, thr_index, n_row, n_col)

    return lax.cond(over, full, fast)


def solution(mesh):
    n_row, n_col = mesh.shape["row"], mesh.shape["col"]
    return jax.shard_map(
        functools.partial(on_device, n_row=n_row, n_col=n_col),
        mesh=mesh,
        in_specs=(P("row", "col"), P("row", "col"), P("row", "col"), P("col")),
        out_specs=P("row", "col"),
        check_vma=False,
    )
```

```python
import functools

import jax
import jax.numpy as jnp
from jax import lax
from jax.experimental import pallas as pl
from jax.experimental.pallas import tpu as pltpu
from jax.sharding import PartitionSpec as P

TB = 128
PAD = 16
AXES = ("row", "col")
F32, BF16, I32 = jnp.float32, jnp.bfloat16, jnp.int32
VMEM = pl.BlockSpec(memory_space=pltpu.VMEM)
SMEM = pl.BlockSpec(memory_space=pltpu.SMEM)


def params(mib):
    return pltpu.CompilerParams(vmem_limit_bytes=mib * 1024 * 1024)


def cost(flops, moved):
    return pl.CostEstimate(flops=int(flops), bytes_accessed=int(moved), transcendentals=0)


def tiles_of(shape):
    return shape[0] // TB, shape[1] // TB


def place():
    col = lax.axis_index("col")
    return lax.axis_index("row"), col // 2, col % 2


def pack_kernel(slots, mask_ref, block_ref, out_ref):
    ti, tj = tiles_of(block_ref.shape)
    lane = lax.broadcasted_iota(I32, (PAD, TB), 1)
    table = jnp.full((PAD, TB), -1, I32)
    used = jnp.int32(0)
    for i in range(ti):
        for j in range(tj):
            stored = mask_ref[j, i]
            fits = jnp.logical_and(stored > 0, used < slots)

            @pl.when(fits)
            def _(i=i, j=j, used=used):
                at = pl.multiple_of(used * TB, TB)
                out_ref[pl.ds(at, TB), :] = block_ref[i * TB : (i + 1) * TB, j * TB : (j + 1) * TB]

            table = jnp.where(lane == i * tj + j, jnp.where(fits, used, -1), table)
            used = used + stored
    table = jnp.where(lane == ti * tj, used, table)
    out_ref[slots * TB :, :] = table.astype(F32).astype(BF16)


def pack(block, mask_t, slots):
    return pl.pallas_call(
        functools.partial(pack_kernel, slots),
        out_shape=jax.ShapeDtypeStruct((slots * TB + PAD, TB), BF16),
        in_specs=[SMEM, VMEM],
        out_specs=VMEM,
        compiler_params=params(8),
        cost_estimate=cost(1e6, 2 * block.size * 2),
        name="pack",
    )(mask_t, block)


def read_tables(blocks, itab, stab, sem):
    for q, parts in enumerate(blocks):
        end = parts[-1].shape[0]
        table = parts[-1][end - PAD : end, :].astype(F32).astype(I32)
        itab[q : q + 1, :] = table[0:1, :]
    copy = pltpu.make_async_copy(itab, stab, sem)
    copy.start()
    copy.wait()


def tile_from(parts, slot):
    def load(ref, at):
        return ref[pl.ds(pl.multiple_of(at * TB, TB), TB), :]

    tile = load(parts[0], jnp.maximum(slot, 0))
    if len(parts) == 2:
        first = parts[0].shape[0] // TB
        tile = load(parts[0], jnp.clip(slot, 0, first - 1))
        tile = jnp.where(slot >= first, load(parts[1], jnp.maximum(slot - first, 0)), tile)
    return jnp.where(slot >= 0, tile, jnp.zeros((TB, TB), BF16))


def table_scratch(n):
    n8 = -(-n // 8) * 8
    return [pltpu.VMEM((n8, TB), I32), pltpu.SMEM((n8, TB), I32), pltpu.SemaphoreType.DMA]


def regroup(refs, sizes):
    out = []
    for s in sizes:
        out.append(refs[:s])
        refs = refs[s:]
    return out


def panel_kernel(slots, sizes, rows, *refs):
    n = len(sizes)
    blocks = regroup(refs, sizes)
    panel_ref, sums_ref, itab, stab, sem = refs[sum(sizes) :]
    cols = panel_ref.shape[1]
    ti, tj = rows // TB, cols // TB
    me = place()[0]
    read_tables(blocks, itab, stab, sem)
    worst = jnp.int32(0)
    sums = tuple(jnp.zeros((8, TB), F32) for _ in range(tj))
    for q in range(n):
        worst = jnp.maximum(worst, stab[q, ti * tj])
        base = (me ^ q) * rows

        def strip(i, sums, q=q, base=base):
            out = []
            for j in range(tj):
                tile = tile_from(blocks[q], stab[q, i * tj + j])
                panel_ref[pl.ds(pl.multiple_of(base + i * TB, TB), TB), j * TB : (j + 1) * TB] = tile
                out.append(sums[j] + jnp.sum(tile.astype(F32).reshape(TB // 8, 8, TB), axis=0))
            return tuple(out)

        sums = lax.fori_loop(0, ti, strip, sums, unroll=2)
    sums_ref[...] = jnp.zeros_like(sums_ref)
    for j in range(tj):
        sums_ref[j : j + 1, :] = jnp.sum(sums[j], axis=0, keepdims=True)
    sums_ref[tj : tj + 1, :] = jnp.full((1, TB), 1.0, F32) * jnp.where(worst > slots, 1.0, 0.0)


def panel(payloads, slots, rows, cols):
    n = len(payloads)
    s_rows = -(-(cols // TB + 1) // 8) * 8
    sizes = [len(p) for p in payloads]
    return pl.pallas_call(
        functools.partial(panel_kernel, slots, sizes, rows),
        out_shape=(
            jax.ShapeDtypeStruct((n * rows, cols), BF16),
            jax.ShapeDtypeStruct((s_rows, TB), F32),
        ),
        in_specs=[VMEM] * sum(sizes),
        out_specs=(VMEM, VMEM),
        scratch_shapes=table_scratch(n),
        compiler_params=params(20),
        cost_estimate=cost(1e7, 2 * n * rows * cols * 2),
        name="panel",
    )(*[x for p in payloads for x in p])


def strip_rows(rows):
    return min(rows, 256)


def unpack_strip(blocks, stab, rows, cols, m, lhs):
    step = strip_rows(rows)
    tj = cols // TB
    for b, parts in enumerate(blocks):
        for a in range(step // TB):
            for j in range(tj):
                tile = tile_from(parts, stab[b, (m * (step // TB) + a) * tj + j])
                lhs[a * TB : (a + 1) * TB, b * cols + j * TB : b * cols + (j + 1) * TB] = tile


def products(blocks, sides, pair, panel_ref, stab, lhs, rows, use):
    cols = panel_ref.shape[1]
    step = strip_rows(rows)
    _, z, core = place()
    n = rows // step
    unpack_strip(blocks, stab, rows, cols, 0, lhs.at[0])
    for m in range(n):
        if m + 1 < n:
            unpack_strip(blocks, stab, rows, cols, m + 1, lhs.at[(m + 1) % 2])
        total = None
        for b, side in enumerate(sides):
            at = pl.multiple_of((z ^ pair) * 2 * cols + (core ^ side) * cols, TB)
            got = jnp.dot(
                lhs[m % 2, :, b * cols : (b + 1) * cols],
                panel_ref[pl.ds(at, cols), :],
                preferred_element_type=F32,
            )
            total = got if total is None else total + got
        use(m, total)


def dot_kernel(n_blocks, sides, pair, rows, has_prior, *refs):
    blocks = regroup(refs, [1] * n_blocks)
    refs = refs[n_blocks:]
    panel_ref = refs[0]
    prior_ref = refs[1] if has_prior else None
    acc_ref, itab, stab, sem, lhs = refs[1 + has_prior :]
    step = strip_rows(rows)
    read_tables(blocks, itab, stab, sem)

    def use(m, got):
        here = slice(m * step, (m + 1) * step)
        acc_ref[here, :] = prior_ref[here, :] + got if has_prior else got

    products(blocks, sides, pair, panel_ref, stab, lhs, rows, use)


def dot_scratch(n, rows, cols):
    return table_scratch(n) + [pltpu.VMEM((2, strip_rows(rows), n * cols), BF16)]


def dots(payloads, sides, pair, dense, prior, rows):
    cols = dense.shape[1]
    n = len(payloads)
    extra = [] if prior is None else [prior]
    return pl.pallas_call(
        functools.partial(dot_kernel, n, sides, pair, rows, len(extra)),
        out_shape=jax.ShapeDtypeStruct((rows, cols), F32),
        in_specs=[VMEM] * (n + 1 + len(extra)),
        out_specs=VMEM,
        scratch_shapes=dot_scratch(n, rows, cols),
        input_output_aliases={n + 1: 0} if extra else {},
        compiler_params=params(20),
        cost_estimate=cost(2 * rows * cols * n * cols, 12 * rows * cols),
        name="dots",
    )(*payloads, dense, *extra)


def means_kernel(n_pairs, s_rows, order, *refs):
    msgs, (thr_ref, panel_ref, out_ref, flag_ref) = refs[:n_pairs], refs[n_pairs:]
    _, z, core = place()
    cols = panel_ref.shape[1]
    tj = cols // TB
    total = jnp.zeros((8, cols), F32)
    row = lax.broadcasted_iota(I32, (8, TB), 0)
    over = jnp.zeros((1, TB), F32)
    for q in range(n_pairs):
        for b in range(2):
            over = jnp.maximum(over, msgs[q][b * s_rows + tj : b * s_rows + tj + 1, :])
            for t in range(tj):
                s = jnp.broadcast_to(msgs[q][b * s_rows + t : b * s_rows + t + 1, :], (8, TB))
                high = s.astype(BF16).astype(F32)
                mid = (s - high).astype(BF16).astype(F32)
                low = s - high - mid
                lhs = jnp.where(row == 0, high, jnp.where(row == 1, mid, jnp.where(row == 2, low, 0.0)))
                at = (z ^ q) * 2 * cols + (core ^ b) * cols + t * TB
                total += jnp.dot(
                    lhs.astype(BF16),
                    panel_ref[pl.ds(pl.multiple_of(at, TB), TB), :],
                    preferred_element_type=F32,
                )
    mean = jnp.sum(total, axis=0, keepdims=True) / order
    out_ref[...] = jnp.broadcast_to(0.125 * thr_ref[...].astype(F32) * mean, out_ref.shape)
    flag_ref[0] = jnp.where(jnp.max(over) > 0.0, 1, 0).astype(I32)


def cuts_of(messages, thr, dense, s_rows, order):
    n = len(messages)
    cols = dense.shape[1]
    return pl.pallas_call(
        functools.partial(means_kernel, n, s_rows, order),
        out_shape=(jax.ShapeDtypeStruct((8, cols), F32), jax.ShapeDtypeStruct((1,), I32)),
        in_specs=[VMEM] * (n + 2),
        out_specs=(VMEM, SMEM),
        compiler_params=params(12),
        cost_estimate=cost(1e7, dense.size * 2),
        name="cuts",
    )(*messages, thr, dense)


def last_kernel(n_blocks, sides, pair, rows, keep_ref, *refs):
    blocks = regroup(refs, [1] * n_blocks)
    panel_ref, prior_ref, cut_ref, acc_ref, tot_ref, itab, stab, sem, lhs = refs[n_blocks:]
    step = strip_rows(rows)
    cols = panel_ref.shape[1]
    read_tables(blocks, itab, stab, sem)
    tot_ref[...] = jnp.zeros_like(tot_ref)
    per = step // TB

    def use(m, got):
        got = prior_ref[m * step : (m + 1) * step, :] + got
        got = jnp.maximum(got - cut_ref[0:1, :], 0.0)
        for a in range(per):
            at = (m * per + a) * TB
            for j in range(cols // TB):
                kept = keep_ref[j, m * per + a].astype(F32)
                cell = got[a * TB : (a + 1) * TB, j * TB : (j + 1) * TB] * kept
                acc_ref[at : at + TB, j * TB : (j + 1) * TB] = cell
                tot_ref[:, j * TB : (j + 1) * TB] += jnp.sum(cell.reshape(TB // 8, 8, TB), axis=0)

    products(blocks, sides, pair, panel_ref, stab, lhs, rows, use)


def finish(keep_t, payloads, sides, pair, dense, prior, cut, rows):
    cols = dense.shape[1]
    n = len(payloads)
    return pl.pallas_call(
        functools.partial(last_kernel, n, sides, pair, rows),
        out_shape=(jax.ShapeDtypeStruct((rows, cols), F32), jax.ShapeDtypeStruct((8, cols), F32)),
        in_specs=[SMEM] + [VMEM] * (n + 3),
        out_specs=(VMEM, VMEM),
        scratch_shapes=dot_scratch(n, rows, cols),
        compiler_params=params(20),
        cost_estimate=cost(2 * rows * cols * n * cols, 12 * rows * cols),
        name="finish",
    )(keep_t, *payloads, dense, prior, cut)


def scale_kernel(n, order, x_ref, *refs):
    tots, out_ref = refs[:n], refs[n]
    total = tots[0][...]
    for t in tots[1:]:
        total = total + t[...]
    total = jnp.sum(total, axis=0, keepdims=True) / order
    factor = 1.0 / jnp.maximum(total, 0.1)
    out_ref[...] = (x_ref[...] * factor).astype(BF16)


def scale(x, totals, order):
    n = len(totals)
    return pl.pallas_call(
        functools.partial(scale_kernel, n, order),
        out_shape=jax.ShapeDtypeStruct(x.shape, BF16),
        in_specs=[VMEM] * (n + 1),
        out_specs=VMEM,
        compiler_params=params(12),
        cost_estimate=cost(2 * x.size, 6 * x.size),
        name="scale",
    )(x, *totals)


def dense_path(values, tile_mask, keep_mask, thr_index, n_row, n_col):
    rows, cols = values.shape
    ti, tj = tiles_of(values.shape)
    matrix = (
        values.reshape(ti, TB, tj, TB) * tile_mask[:, None, :, None].astype(BF16)
    ).reshape(rows, cols)
    kept = jnp.broadcast_to(keep_mask[:, None, :, None].astype(F32), (ti, TB, tj, TB)).reshape(rows, cols)
    r, c = lax.axis_index("row"), lax.axis_index("col")
    order = rows * n_row

    def col_ring(i, carry):
        block, panel_ = carry
        panel_ = lax.dynamic_update_slice(panel_, block, (((r - i) % n_row) * rows, 0))
        return lax.ppermute(block, "row", [(k, (k + 1) % n_row) for k in range(n_row)]), panel_

    _, panel_ = lax.fori_loop(0, n_row, col_ring, (matrix, jnp.zeros((order, cols), BF16)))

    def row_ring(i, carry):
        block, acc = carry
        part = lax.dynamic_slice(panel_, (((c - i) % n_col) * cols, 0), (cols, cols))
        acc = acc + jnp.dot(block, part, preferred_element_type=F32)
        return lax.ppermute(block, "col", [(k, (k + 1) % n_col) for k in range(n_col)]), acc

    _, product = lax.fori_loop(0, n_col, row_ring, (matrix, jnp.zeros((rows, cols), F32)))
    means = lax.psum(jnp.sum(product, axis=0), "row") / order
    pruned = jnp.maximum(product - 0.125 * thr_index.astype(F32) * means, 0.0) * kept
    totals = lax.psum(jnp.sum(pruned, axis=0), "row") / order
    return (pruned / jnp.maximum(totals, 0.1)).astype(BF16)


def on_device(values, tile_mask, keep_mask, thr_index, n_row, n_col):
    return body(values, tile_mask, keep_mask, thr_index, n_row, n_col)


def body(values, tile_mask, keep_mask, thr_index, n_row, n_col):
    rows, cols = values.shape
    ti, tj = tiles_of(values.shape)
    slots = ti * tj * 3 // 4
    half = slots // 2 * TB
    n_z = n_col // 2
    last = n_z - 1
    order = rows * n_row

    def send(x, dr=0, dz=0, dc=0):
        pairs = [
            (r * n_col + z * 2 + c, (r ^ dr) * n_col + (z ^ dz) * 2 + (c ^ dc))
            for r in range(n_row)
            for z in range(n_z)
            for c in range(2)
        ]
        return lax.ppermute(x, AXES, pairs)

    own = pack(values, tile_mask.T, slots)

    line = {0: own}
    for j in range(1, n_z):
        low = j & -j
        line[j] = send(line[j ^ low], dz=low)
    swapped = {j: send(line[j], dc=1) for j in range(n_z)}

    column = {0: [own]}
    for q in range(1, n_row):
        low = q & -q
        rest = q ^ low
        if rest and rest & -rest == rest:
            column[q] = [send(column[low][0][:half], dr=rest), send(column[rest][0][half:], dr=low)]
        else:
            column[q] = [send(own, dr=q)]

    dense, sums = panel([column[q] for q in range(n_row)], slots, rows, cols)
    acc = None
    for j in range(last):
        acc = dots([line[j], swapped[j]], (0, 1), j, dense, acc, rows)
    acc = dots([line[last]], (0,), last, dense, acc, rows)

    both = jnp.concatenate([sums, send(sums, dc=1)], axis=0)
    messages = [both] + [send(both, dz=j) for j in range(1, n_z)]
    cut, over = cuts_of(messages, thr_index.reshape(1, cols), dense, sums.shape[0], order)

    def fast():
        pruned, tot = finish(keep_mask.T, [swapped[last]], (1,), last, dense, acc, cut, rows)
        totals = [tot] + [send(tot, dr=q) for q in range(1, n_row)]
        return scale(pruned, totals, order)

    def full():
        return dense_path(values, tile_mask, keep_mask, thr_index, n_row, n_col)

    return lax.cond(over[0] > 0, full, fast)


def solution(mesh):
    n_row, n_col = mesh.shape["row"], mesh.shape["col"]
    return jax.shard_map(
        functools.partial(on_device, n_row=n_row, n_col=n_col),
        mesh=mesh,
        in_specs=(P("row", "col"), P("row", "col"), P("row", "col"), P("col")),
        out_specs=P("row", "col"),
        check_vma=False,
    )
```

```python
import functools

import jax
import jax.numpy as jnp
from jax import lax
from jax.experimental import pallas as pl
from jax.experimental.pallas import tpu as pltpu
from jax.sharding import PartitionSpec as P

TB = 128
PAD = 16
AXES = ("row", "col")
F32, BF16, I32 = jnp.float32, jnp.bfloat16, jnp.int32
VMEM = pl.BlockSpec(memory_space=pltpu.VMEM)
SMEM = pl.BlockSpec(memory_space=pltpu.SMEM)


def params(mib):
    return pltpu.CompilerParams(vmem_limit_bytes=mib * 1024 * 1024)


def cost(flops, moved):
    return pl.CostEstimate(flops=int(flops), bytes_accessed=int(moved), transcendentals=0)


def tiles_of(shape):
    return shape[0] // TB, shape[1] // TB


def place():
    col = lax.axis_index("col")
    return lax.axis_index("row"), col // 2, col % 2


def table_of(ref):
    end = ref.shape[0]
    return ref[end - PAD : end, :].astype(F32).astype(I32)[0:1, :]


def pack_kernel(mask_ref, block_ref, out_ref, head_ref):
    ti, tj = tiles_of(block_ref.shape)
    slots, first = (out_ref.shape[0] - PAD) // TB, (head_ref.shape[0] - PAD) // TB
    lane = lax.broadcasted_iota(I32, (PAD, TB), 1)
    table = jnp.full((PAD, TB), -1, I32)
    used = jnp.int32(0)
    for i in range(ti):
        for j in range(tj):
            stored = mask_ref[j, i]

            @pl.when(jnp.logical_and(stored > 0, used < slots))
            def _(i=i, j=j, used=used):
                tile = block_ref[i * TB : (i + 1) * TB, j * TB : (j + 1) * TB]
                here = pl.ds(pl.multiple_of(used * TB, TB), TB)
                out_ref[here, :] = tile

                @pl.when(used < first)
                def _():
                    head_ref[here, :] = tile

            table = jnp.where(lane == i * tj + j, jnp.where(stored > 0, used, -1), table)
            used = used + stored
    table = jnp.where(lane == ti * tj, used, table).astype(F32).astype(BF16)
    out_ref[slots * TB :, :] = table
    head_ref[first * TB :, :] = table


def pack(block, mask_t, slots, first):
    return pl.pallas_call(
        pack_kernel,
        out_shape=tuple(jax.ShapeDtypeStruct((n * TB + PAD, TB), BF16) for n in (slots, first)),
        in_specs=[SMEM, VMEM],
        out_specs=(VMEM, VMEM),
        compiler_params=params(8),
        cost_estimate=cost(1e6, 2 * block.size * 2),
        name="pack",
    )(mask_t, block)


def load(ref, at, count):
    return ref[pl.ds(pl.multiple_of(jnp.clip(at, 0, count - 1) * TB, TB), TB), :]


def pool_kernel(first, mask_ref, block_ref, own_ref, other_ref, out_ref, msg_ref):
    ti, tj = tiles_of(block_ref.shape)
    slots, n = (own_ref.shape[0] - PAD) // TB, out_ref.shape[0] // TB
    core = place()[2]
    count = jnp.int32(0)
    sums = [jnp.zeros((8, TB), F32) for _ in range(tj)]
    for i in range(ti):
        for j in range(tj):
            stored = mask_ref[j, i]
            count = count + stored
            tile = block_ref[i * TB : (i + 1) * TB, j * TB : (j + 1) * TB].astype(F32)
            sums[j] += jnp.sum(tile.reshape(TB // 8, 8, TB), axis=0) * stored.astype(F32)
    lane = lax.broadcasted_iota(I32, (1, TB), 1)
    theirs = jnp.max(jnp.where(lane == ti * tj, table_of(other_ref), 0))
    left = jnp.maximum(count - first, 0)
    left_other = jnp.maximum(theirs - first, 0)
    left_0 = jnp.where(core == 0, left, left_other)
    for i in range(n):
        p = core * n + i
        in_0 = p < left_0
        at = first + jnp.where(in_0, p, p - left_0)
        mine = jnp.where(in_0, 0, 1) == core
        tile = jnp.where(mine, load(own_ref, at, slots), load(other_ref, at, slots))
        out_ref[i * TB : (i + 1) * TB, :] = tile
    over = jnp.logical_or(count > slots, left + left_other > 2 * n)
    msg_ref[...] = jnp.zeros_like(msg_ref)
    for j in range(tj):
        msg_ref[j : j + 1, :] = jnp.sum(sums[j], axis=0, keepdims=True)
    msg_ref[tj : tj + 1, :] = jnp.full((1, TB), 1.0, F32) * jnp.where(over, 1.0, 0.0)


def pool(block, mask_t, own, other, first, n):
    s_rows = -(-(block.shape[1] // TB + 1) // 8) * 8
    return pl.pallas_call(
        functools.partial(pool_kernel, first),
        out_shape=(
            jax.ShapeDtypeStruct((n * TB, TB), BF16),
            jax.ShapeDtypeStruct((s_rows, TB), F32),
        ),
        in_specs=[SMEM] + [VMEM] * 3,
        out_specs=(VMEM, VMEM),
        compiler_params=params(8),
        cost_estimate=cost(1e6, 2 * block.size * 2),
        name="pool",
    )(mask_t, block, own, other)


def read_tables(refs, itab, stab, sem):
    for q, ref in enumerate(refs):
        itab[q : q + 1, :] = table_of(ref)
    copy = pltpu.make_async_copy(itab, stab, sem)
    copy.start()
    copy.wait()


def zero_tile():
    return jnp.zeros((TB, TB), BF16)


def whole_tile(parts, slots, at):
    first = parts[0].shape[0] // TB if len(parts) == 2 else slots
    tile = load(parts[0], at, first)
    if len(parts) == 2:
        tile = jnp.where(at >= first, load(parts[1], at - first, slots - first), tile)
    return jnp.where(at >= 0, tile, zero_tile())


def table_scratch(n):
    n8 = -(-n // 8) * 8
    return [pltpu.VMEM((n8, TB), I32), pltpu.SMEM((n8, TB), I32), pltpu.SemaphoreType.DMA]


def regroup(refs, sizes):
    out = []
    for s in sizes:
        out.append(refs[:s])
        refs = refs[s:]
    return out


def panel_kernel(slots, sizes, rows, *refs):
    blocks = regroup(refs, sizes)
    panel_ref, itab, stab, sem = refs[sum(sizes) :]
    cols = panel_ref.shape[1]
    ti, tj = rows // TB, cols // TB
    me = place()[0]
    read_tables([b[-1] for b in blocks], itab, stab, sem)
    for q in range(len(sizes)):
        base = (me ^ q) * rows

        def strip(i, done, q=q, base=base):
            for j in range(tj):
                tile = whole_tile(blocks[q], slots, stab[q, i * tj + j])
                panel_ref[pl.ds(pl.multiple_of(base + i * TB, TB), TB), j * TB : (j + 1) * TB] = tile
            return done

        lax.fori_loop(0, ti, strip, 0, unroll=2)


def panel(payloads, slots, rows, cols):
    n = len(payloads)
    sizes = [len(p) for p in payloads]
    return pl.pallas_call(
        functools.partial(panel_kernel, slots, sizes, rows),
        out_shape=jax.ShapeDtypeStruct((n * rows, cols), BF16),
        in_specs=[VMEM] * sum(sizes),
        out_specs=VMEM,
        scratch_shapes=table_scratch(n),
        compiler_params=params(20),
        cost_estimate=cost(1e7, 2 * n * rows * cols * 2),
        name="panel",
    )(*[x for p in payloads for x in p])


def strip_rows(rows):
    return min(rows, 256)


def tile_getters(kind, refs, stab, tiles, core):
    if kind == "whole":
        slots = (refs[0].shape[0] - PAD) // TB
        return [lambda at, r=r: whole_tile([r], slots, at) for r in refs]
    first = (refs[0].shape[0] - PAD) // TB
    if kind == "heads":
        return [
            lambda at, r=r: jnp.where(
                jnp.logical_and(at >= 0, at < first), load(r, at, first), zero_tile()
            )
            for r in refs
        ]
    n = refs[2].shape[0] // TB
    left = [jnp.maximum(stab[b, tiles] - first, 0) for b in range(2)]
    left_0 = jnp.where(core == 0, left[0], left[1])

    def getter(side):
        base = jnp.where((core ^ side) == 1, left_0, 0) - first

        def get(at):
            p = at + base
            part = jnp.where(p >= n, 1, 0)
            local = p - part * n
            rest = jnp.where(part == core, load(refs[2], local, n), load(refs[3], local, n))
            if kind == "pools":
                return jnp.where(at >= first, rest, zero_tile())
            tile = jnp.where(at >= first, rest, load(refs[side], at, first))
            return jnp.where(at >= 0, tile, zero_tile())

        return get

    return [getter(0), getter(1)]


def products(kind, refs, pair, panel_ref, itab, stab, sem, lhs, rows, use):
    cols = panel_ref.shape[1]
    step = strip_rows(rows)
    tj = cols // TB
    _, z, core = place()
    read_tables(refs[:2], itab, stab, sem)
    getters = tile_getters(kind, refs, stab, rows // TB * tj, core)
    n = rows // step
    start = (refs[0].shape[0] - PAD) // TB // tj * TB // step if kind == "pools" else 0

    def unpack(m):
        for b, get in enumerate(getters):
            for a in range(step // TB):
                for j in range(tj):
                    tile = get(stab[b, (m * (step // TB) + a) * tj + j])
                    lhs[m % 2, a * TB : (a + 1) * TB, b * cols + j * TB : b * cols + (j + 1) * TB] = tile

    unpack(start)
    for m in range(start):
        use(m, None)
    for m in range(start, n):
        if m + 1 < n:
            unpack(m + 1)
        total = None
        for b in range(2):
            at = pl.multiple_of((z ^ pair) * 2 * cols + (core ^ b) * cols, TB)
            got = jnp.dot(
                lhs[m % 2, :, b * cols : (b + 1) * cols],
                panel_ref[pl.ds(at, cols), :],
                preferred_element_type=F32,
            )
            total = got if total is None else total + got
        use(m, total)


def dot_kernel(kind, n, pair, rows, has_prior, *refs):
    panel_ref = refs[n]
    prior_ref = refs[n + 1] if has_prior else None
    acc_ref, itab, stab, sem, lhs = refs[n + 1 + has_prior :]
    step = strip_rows(rows)

    def use(m, got):
        here = slice(m * step, (m + 1) * step)
        acc_ref[here, :] = prior_ref[here, :] + got if has_prior else got

    products(kind, refs[:n], pair, panel_ref, itab, stab, sem, lhs, rows, use)


def dot_scratch(rows, cols):
    return table_scratch(2) + [pltpu.VMEM((2, strip_rows(rows), 2 * cols), BF16)]


def dots(kind, payloads, pair, dense, prior, rows):
    cols = dense.shape[1]
    n = len(payloads)
    extra = [] if prior is None else [prior]
    return pl.pallas_call(
        functools.partial(dot_kernel, kind, n, pair, rows, len(extra)),
        out_shape=jax.ShapeDtypeStruct((rows, cols), F32),
        in_specs=[VMEM] * (n + 1 + len(extra)),
        out_specs=VMEM,
        scratch_shapes=dot_scratch(rows, cols),
        input_output_aliases={n + 1: 0} if extra else {},
        compiler_params=params(20),
        cost_estimate=cost(4 * rows * cols * cols, 12 * rows * cols),
        name="dots",
    )(*payloads, dense, *extra)


def means_kernel(n_pairs, s_rows, order, *refs):
    msgs, (thr_ref, panel_ref, out_ref, flag_ref) = refs[:n_pairs], refs[n_pairs:]
    _, z, core = place()
    cols = panel_ref.shape[1]
    tj = cols // TB
    total = jnp.zeros((8, cols), F32)
    row = lax.broadcasted_iota(I32, (8, TB), 0)
    over = jnp.zeros((1, TB), F32)
    for q in range(n_pairs):
        for b in range(2):
            over = jnp.maximum(over, msgs[q][b * s_rows + tj : b * s_rows + tj + 1, :])
            for t in range(tj):
                s = jnp.broadcast_to(msgs[q][b * s_rows + t : b * s_rows + t + 1, :], (8, TB))
                high = s.astype(BF16).astype(F32)
                mid = (s - high).astype(BF16).astype(F32)
                low = s - high - mid
                lhs = jnp.where(row == 0, high, jnp.where(row == 1, mid, jnp.where(row == 2, low, 0.0)))
                at = (z ^ q) * 2 * cols + (core ^ b) * cols + t * TB
                total += jnp.dot(
                    lhs.astype(BF16),
                    panel_ref[pl.ds(pl.multiple_of(at, TB), TB), :],
                    preferred_element_type=F32,
                )
    mean = jnp.sum(total, axis=0, keepdims=True) / order
    out_ref[...] = jnp.broadcast_to(0.125 * thr_ref[...].astype(F32) * mean, out_ref.shape)
    flag_ref[0] = jnp.where(jnp.max(over) > 0.0, 1, 0).astype(I32)


def cuts_of(messages, thr, dense, s_rows, order):
    n = len(messages)
    cols = dense.shape[1]
    return pl.pallas_call(
        functools.partial(means_kernel, n, s_rows, order),
        out_shape=(jax.ShapeDtypeStruct((8, cols), F32), jax.ShapeDtypeStruct((1,), I32)),
        in_specs=[VMEM] * (n + 2),
        out_specs=(VMEM, SMEM),
        compiler_params=params(12),
        cost_estimate=cost(1e7, dense.size * 2),
        name="cuts",
    )(*messages, thr, dense)


def last_kernel(kind, n, pair, rows, keep_ref, *refs):
    panel_ref, prior_ref, cut_ref, acc_ref, tot_ref, itab, stab, sem, lhs = refs[n:]
    step = strip_rows(rows)
    cols = panel_ref.shape[1]
    per = step // TB
    totals = [jnp.zeros((8, TB), F32) for _ in range(cols // TB)]

    def use(m, got):
        prior = prior_ref[m * step : (m + 1) * step, :]
        got = jnp.maximum((prior if got is None else prior + got) - cut_ref[0:1, :], 0.0)
        for a in range(per):
            at = (m * per + a) * TB
            for j in range(cols // TB):
                kept = keep_ref[j, m * per + a].astype(F32)
                cell = got[a * TB : (a + 1) * TB, j * TB : (j + 1) * TB] * kept
                acc_ref[at : at + TB, j * TB : (j + 1) * TB] = cell
                totals[j] += jnp.sum(cell.reshape(TB // 8, 8, TB), axis=0)

    products(kind, refs[:n], pair, panel_ref, itab, stab, sem, lhs, rows, use)
    for j, t in enumerate(totals):
        tot_ref[:, j * TB : (j + 1) * TB] = jnp.sum(t, axis=0, keepdims=True)


def finish(kind, keep_t, payloads, pair, dense, prior, cut, rows):
    cols = dense.shape[1]
    n = len(payloads)
    return pl.pallas_call(
        functools.partial(last_kernel, kind, n, pair, rows),
        out_shape=(jax.ShapeDtypeStruct((rows, cols), F32), jax.ShapeDtypeStruct((1, cols), F32)),
        in_specs=[SMEM] + [VMEM] * (n + 3),
        out_specs=(VMEM, VMEM),
        scratch_shapes=dot_scratch(rows, cols),
        compiler_params=params(20),
        cost_estimate=cost(4 * rows * cols * cols, 12 * rows * cols),
        name="finish",
    )(keep_t, *payloads, dense, prior, cut)


def scale_kernel(n, order, x_ref, *refs):
    tots, out_ref = refs[:n], refs[n]
    total = tots[0][...]
    for t in tots[1:]:
        total = total + t[...]
    total = total / order
    factor = 1.0 / jnp.maximum(total, 0.1)
    out_ref[...] = (x_ref[...] * factor).astype(BF16)


def scale(x, totals, order):
    n = len(totals)
    return pl.pallas_call(
        functools.partial(scale_kernel, n, order),
        out_shape=jax.ShapeDtypeStruct(x.shape, BF16),
        in_specs=[VMEM] * (n + 1),
        out_specs=VMEM,
        compiler_params=params(12),
        cost_estimate=cost(2 * x.size, 6 * x.size),
        name="scale",
    )(x, *totals)


def dense_path(values, tile_mask, keep_mask, thr_index, n_row, n_col):
    rows, cols = values.shape
    ti, tj = tiles_of(values.shape)
    matrix = (
        values.reshape(ti, TB, tj, TB) * tile_mask[:, None, :, None].astype(BF16)
    ).reshape(rows, cols)
    kept = jnp.broadcast_to(keep_mask[:, None, :, None].astype(F32), (ti, TB, tj, TB)).reshape(rows, cols)
    r, c = lax.axis_index("row"), lax.axis_index("col")
    order = rows * n_row

    def col_ring(i, carry):
        block, panel_ = carry
        panel_ = lax.dynamic_update_slice(panel_, block, (((r - i) % n_row) * rows, 0))
        return lax.ppermute(block, "row", [(k, (k + 1) % n_row) for k in range(n_row)]), panel_

    _, panel_ = lax.fori_loop(0, n_row, col_ring, (matrix, jnp.zeros((order, cols), BF16)))

    def row_ring(i, carry):
        block, acc = carry
        part = lax.dynamic_slice(panel_, (((c - i) % n_col) * cols, 0), (cols, cols))
        acc = acc + jnp.dot(block, part, preferred_element_type=F32)
        return lax.ppermute(block, "col", [(k, (k + 1) % n_col) for k in range(n_col)]), acc

    _, product = lax.fori_loop(0, n_col, row_ring, (matrix, jnp.zeros((rows, cols), F32)))
    means = lax.psum(jnp.sum(product, axis=0), "row") / order
    pruned = jnp.maximum(product - 0.125 * thr_index.astype(F32) * means, 0.0) * kept
    totals = lax.psum(jnp.sum(pruned, axis=0), "row") / order
    return (pruned / jnp.maximum(totals, 0.1)).astype(BF16)


def on_device(values, tile_mask, keep_mask, thr_index, n_row, n_col):
    return body(values, tile_mask, keep_mask, thr_index, n_row, n_col)


def body(values, tile_mask, keep_mask, thr_index, n_row, n_col):
    rows, cols = values.shape
    ti, tj = tiles_of(values.shape)
    first = ti * tj // 2
    extra = ti * tj * 3 // 16
    slots = ti * tj * 13 // 16
    half = slots // 2 * TB
    n_z = n_col // 2
    last = n_z - 1
    order = rows * n_row

    def send(x, dr=0, dz=0, dc=0):
        pairs = [
            (r * n_col + z * 2 + c, (r ^ dr) * n_col + (z ^ dz) * 2 + (c ^ dc))
            for r in range(n_row)
            for z in range(n_z)
            for c in range(2)
        ]
        return lax.ppermute(x, AXES, pairs)

    own, head = pack(values, tile_mask.T, slots, first)
    own_swapped = send(own, dc=1)
    spare, sums = pool(values, tile_mask.T, own, own_swapped, first, extra)

    line = {0: [head, spare]}
    swapped = {}
    for j in range(1, n_z):
        low = j & -j
        line[j] = [send(x, dz=low) for x in line[j ^ low]]
        swapped[j] = [send(x, dc=1) for x in line[j]]

    column = {0: [own]}
    for q in range(1, n_row):
        low = q & -q
        rest = q ^ low
        if rest and rest & -rest == rest:
            column[q] = [send(column[low][0][:half], dr=rest), send(column[rest][0][half:], dr=low)]
        else:
            column[q] = [send(own, dr=q)]

    dense = panel([column[q] for q in range(n_row)], slots, rows, cols)

    sums = functools.reduce(jnp.add, [send(sums, dr=q) for q in range(1, n_row)], sums)
    both = jnp.concatenate([sums, send(sums, dc=1)], axis=0)
    messages = [both] + [send(both, dz=j) for j in range(1, n_z)]
    cut, over = cuts_of(messages, thr_index.reshape(1, cols), dense, sums.shape[0], order)

    acc = None
    for j in range(n_z):
        if j == 0:
            acc = dots("whole", [own, own_swapped], j, dense, acc, rows)
        elif j < last:
            parts = [line[j][0], swapped[j][0], line[j][1], swapped[j][1]]
            acc = dots("all", parts, j, dense, acc, rows)
        else:
            acc = dots("heads", [line[j][0], swapped[j][0]], j, dense, acc, rows)

    def fast():
        parts = [line[last][0], swapped[last][0], line[last][1], swapped[last][1]]
        pruned, tot = finish("pools", keep_mask.T, parts, last, dense, acc, cut, rows)
        totals = [tot] + [send(tot, dr=q) for q in range(1, n_row)]
        return scale(pruned, totals, order)

    def full():
        return dense_path(values, tile_mask, keep_mask, thr_index, n_row, n_col)

    return lax.cond(over[0] > 0, full, fast)


def solution(mesh):
    n_row, n_col = mesh.shape["row"], mesh.shape["col"]
    return jax.shard_map(
        functools.partial(on_device, n_row=n_row, n_col=n_col),
        mesh=mesh,
        in_specs=(P("row", "col"), P("row", "col"), P("row", "col"), P("col")),
        out_specs=P("row", "col"),
        check_vma=False,
    )
```

```python
import functools

import jax
import jax.numpy as jnp
from jax import lax
from jax.experimental import pallas as pl
from jax.experimental.pallas import tpu as pltpu
from jax.sharding import PartitionSpec as P

TB = 128
PAD = 16
AXES = ("row", "col")
F32, BF16, I32 = jnp.float32, jnp.bfloat16, jnp.int32
VMEM = pl.BlockSpec(memory_space=pltpu.VMEM)
SMEM = pl.BlockSpec(memory_space=pltpu.SMEM)


def params(mib):
    return pltpu.CompilerParams(vmem_limit_bytes=mib * 1024 * 1024)


def cost(flops, moved):
    return pl.CostEstimate(flops=int(flops), bytes_accessed=int(moved), transcendentals=0)


def tiles_of(shape):
    return shape[0] // TB, shape[1] // TB


def place():
    col = lax.axis_index("col")
    return lax.axis_index("row"), col // 2, col % 2


def table_of(ref):
    end = ref.shape[0]
    return ref[end - PAD : end, :].astype(F32).astype(I32)[0:1, :]


def places(ref):
    return (ref.shape[0] - PAD) // TB


def pack_kernel(mask_ref, block_ref, head_ref, rest_ref):
    ti, tj = tiles_of(block_ref.shape)
    first, slots = places(head_ref), places(head_ref) + places(rest_ref)
    lane = lax.broadcasted_iota(I32, (PAD, TB), 1)
    table = jnp.full((PAD, TB), -1, I32)
    used = jnp.int32(0)
    for i in range(ti):
        for j in range(tj):
            stored = mask_ref[j, i]

            @pl.when(jnp.logical_and(stored > 0, used < first))
            def _(i=i, j=j, used=used):
                tile = block_ref[i * TB : (i + 1) * TB, j * TB : (j + 1) * TB]
                head_ref[pl.ds(pl.multiple_of(used * TB, TB), TB), :] = tile

            if i * tj + j >= first:

                @pl.when(jnp.logical_and(stored > 0, jnp.logical_and(used >= first, used < slots)))
                def _(i=i, j=j, used=used):
                    tile = block_ref[i * TB : (i + 1) * TB, j * TB : (j + 1) * TB]
                    rest_ref[pl.ds(pl.multiple_of((used - first) * TB, TB), TB), :] = tile

            table = jnp.where(lane == i * tj + j, jnp.where(stored > 0, used, -1), table)
            used = used + stored
    table = jnp.where(lane == ti * tj, used, table).astype(F32).astype(BF16)
    head_ref[first * TB :, :] = table
    rest_ref[(slots - first) * TB :, :] = table


def pack(block, mask_t, slots, first):
    return pl.pallas_call(
        pack_kernel,
        out_shape=tuple(jax.ShapeDtypeStruct((n * TB + PAD, TB), BF16) for n in (first, slots - first)),
        in_specs=[SMEM, VMEM],
        out_specs=(VMEM, VMEM),
        compiler_params=params(8),
        cost_estimate=cost(1e6, 2 * block.size * 2),
        name="pack",
    )(mask_t, block)


def load(ref, at, count):
    return ref[pl.ds(pl.multiple_of(jnp.clip(at, 0, count - 1) * TB, TB), TB), :]


def pool_kernel(first, mask_ref, block_ref, rest_ref, other_ref, out_ref, msg_ref):
    ti, tj = tiles_of(block_ref.shape)
    spare, n = places(rest_ref), out_ref.shape[0] // TB
    core = place()[2]
    count = jnp.int32(0)
    sums = [jnp.zeros((8, TB), F32) for _ in range(tj)]
    for i in range(ti):
        for j in range(tj):
            stored = mask_ref[j, i]
            count = count + stored
            tile = block_ref[i * TB : (i + 1) * TB, j * TB : (j + 1) * TB].astype(F32)
            sums[j] += jnp.sum(tile.reshape(TB // 8, 8, TB), axis=0) * stored.astype(F32)
    lane = lax.broadcasted_iota(I32, (1, TB), 1)
    theirs = jnp.max(jnp.where(lane == ti * tj, table_of(other_ref), 0))
    left = jnp.maximum(count - first, 0)
    left_other = jnp.maximum(theirs - first, 0)
    left_0 = jnp.where(core == 0, left, left_other)
    for i in range(n):
        p = core * n + i
        in_0 = p < left_0
        at = jnp.where(in_0, p, p - left_0)
        mine = jnp.where(in_0, 0, 1) == core
        tile = jnp.where(mine, load(rest_ref, at, spare), load(other_ref, at, spare))
        out_ref[i * TB : (i + 1) * TB, :] = tile
    over = jnp.logical_or(left > spare, left + left_other > 2 * n)
    msg_ref[...] = jnp.zeros_like(msg_ref)
    for j in range(tj):
        msg_ref[j : j + 1, :] = jnp.sum(sums[j], axis=0, keepdims=True)
    msg_ref[tj : tj + 1, :] = jnp.full((1, TB), 1.0, F32) * jnp.where(over, 1.0, 0.0)


def pool(block, mask_t, rest, other, first, n):
    s_rows = -(-(block.shape[1] // TB + 1) // 8) * 8
    return pl.pallas_call(
        functools.partial(pool_kernel, first),
        out_shape=(
            jax.ShapeDtypeStruct((n * TB, TB), BF16),
            jax.ShapeDtypeStruct((s_rows, TB), F32),
        ),
        in_specs=[SMEM] + [VMEM] * 3,
        out_specs=(VMEM, VMEM),
        compiler_params=params(8),
        cost_estimate=cost(1e6, 2 * block.size * 2),
        name="pool",
    )(mask_t, block, rest, other)


def read_tables(refs, itab, stab, sem):
    for q, ref in enumerate(refs):
        itab[q : q + 1, :] = table_of(ref)
    copy = pltpu.make_async_copy(itab, stab, sem)
    copy.start()
    copy.wait()


def zero_tile():
    return jnp.zeros((TB, TB), BF16)


def whole_tile(parts, at, low):
    first = places(parts[0])
    tile = load(parts[0], at, first)
    if not low:
        tile = jnp.where(at >= first, load(parts[1], at - first, places(parts[1])), tile)
    return jnp.where(at >= 0, tile, zero_tile())


def table_scratch(n):
    n8 = -(-n // 8) * 8
    return [pltpu.VMEM((n8, TB), I32), pltpu.SMEM((n8, TB), I32), pltpu.SemaphoreType.DMA]


def regroup(refs, sizes):
    out = []
    for s in sizes:
        out.append(refs[:s])
        refs = refs[s:]
    return out


def strip_rows(rows):
    return min(rows, 256)


def tile_getters(kind, refs, stab, at_table, tiles, core):
    first = places(refs[0])
    if kind == "whole":
        return [lambda at, low, b=b: whole_tile((refs[b], refs[2 + b]), at, low) for b in range(2)]

    def head(side, at):
        return jnp.where(
            jnp.logical_and(at >= 0, at < first), load(refs[side], at, first), zero_tile()
        )

    if kind == "heads":
        return [lambda at, low, b=b: head(b, at) for b in range(2)]
    n = refs[2].shape[0] // TB
    left = [jnp.maximum(stab[at_table[b], tiles] - first, 0) for b in range(2)]
    left_0 = jnp.where(core == 0, left[0], left[1])

    def getter(side):
        base = jnp.where((core ^ side) == 1, left_0, 0) - first

        def get(at, low):
            if low:
                return head(side, at)
            p = at + base
            part = jnp.where(p >= n, 1, 0)
            local = p - part * n
            rest = jnp.where(part == core, load(refs[2], local, n), load(refs[3], local, n))
            if kind == "pools":
                return jnp.where(at >= first, rest, zero_tile())
            return jnp.where(at >= first, rest, head(side, at))

        return get

    return [getter(0), getter(1)]


def products(kind, refs, pair, panel_ref, stab, at_table, lhs, rows, use):
    cols = panel_ref.shape[1]
    step = strip_rows(rows)
    tj = cols // TB
    _, z, core = place()
    getters = tile_getters(kind, refs, stab, at_table, rows // TB * tj, core)
    n = rows // step
    safe = places(refs[0]) // tj
    start = safe * TB // step if kind == "pools" else 0

    def unpack(m):
        for b, get in enumerate(getters):
            for a in range(step // TB):
                i = m * (step // TB) + a
                tiles = [get(stab[at_table[b], i * tj + j], i < safe) for j in range(tj)]
                lhs[m % 2, a * TB : (a + 1) * TB, b * cols : (b + 1) * cols] = jnp.concatenate(tiles, axis=1)

    unpack(start)
    for m in range(start):
        use(m, None)
    for m in range(start, n):
        if m + 1 < n:
            unpack(m + 1)
        total = None
        for b in range(2):
            at = pl.multiple_of((z ^ pair) * 2 * cols + (core ^ b) * cols, TB)
            got = jnp.dot(
                lhs[m % 2, :, b * cols : (b + 1) * cols],
                panel_ref[pl.ds(at, cols), :],
                preferred_element_type=F32,
            )
            total = got if total is None else total + got
        use(m, total)


def adder(acc_ref, prior_ref, rows):
    step = strip_rows(rows)

    def use(m, got):
        here = slice(m * step, (m + 1) * step)
        acc_ref[here, :] = got if prior_ref is None else prior_ref[here, :] + got

    return use


def dot_scratch(n, rows, cols):
    return table_scratch(n) + [pltpu.VMEM((2, strip_rows(rows), 2 * cols), BF16)]


def panel_kernel(n, rows, *refs):
    blocks, other = regroup(refs, [2] * n), refs[2 * n : 2 * n + 2]
    panel_ref, acc_ref, itab, stab, sem, lhs = refs[2 * n + 2 :]
    cols = panel_ref.shape[1]
    ti, tj = rows // TB, cols // TB
    me = place()[0]
    read_tables([b[1] for b in blocks] + [other[1]], itab, stab, sem)
    safe = places(blocks[0][0]) // tj
    for q in range(n):
        base = (me ^ q) * rows

        def strip(i, done, q=q, base=base, low=False):
            tiles = [whole_tile(blocks[q], stab[q, i * tj + j], low) for j in range(tj)]
            panel_ref[pl.ds(pl.multiple_of(base + i * TB, TB), TB), :] = jnp.concatenate(tiles, axis=1)
            return done

        lax.fori_loop(0, safe, functools.partial(strip, low=True), 0, unroll=2)
        lax.fori_loop(safe, ti, strip, 0, unroll=2)
    mine = blocks[0]
    heads_rests = (mine[0], other[0], mine[1], other[1])
    products("whole", heads_rests, 0, panel_ref, stab, (0, n), lhs, rows, adder(acc_ref, None, rows))


def panel(payloads, other, rows, cols):
    n = len(payloads)
    return pl.pallas_call(
        functools.partial(panel_kernel, n, rows),
        out_shape=(
            jax.ShapeDtypeStruct((n * rows, cols), BF16),
            jax.ShapeDtypeStruct((rows, cols), F32),
        ),
        in_specs=[VMEM] * (2 * n + 2),
        out_specs=(VMEM, VMEM),
        scratch_shapes=dot_scratch(n + 1, rows, cols),
        compiler_params=params(24),
        cost_estimate=cost(4 * rows * cols * cols, 2 * n * rows * cols * 2),
        name="panel",
    )(*[x for p in payloads for x in p], *other)


def dot_kernel(kind, pairs, rows, *refs):
    per = 4 if kind == "all" else 2
    blocks = regroup(refs, [per] * len(pairs))
    panel_ref, prior_ref, acc_ref, itab, stab, sem, lhs = refs[per * len(pairs) :]
    read_tables([r for b in blocks for r in b[:2]], itab, stab, sem)
    for k, (pair, b) in enumerate(zip(pairs, blocks)):
        use = adder(acc_ref, acc_ref if k else prior_ref, rows)
        products(kind, b, pair, panel_ref, stab, (2 * k, 2 * k + 1), lhs, rows, use)


def dots(kind, blocks, pairs, dense, prior, rows):
    cols = dense.shape[1]
    flat = [x for b in blocks for x in b]
    return pl.pallas_call(
        functools.partial(dot_kernel, kind, pairs, rows),
        out_shape=jax.ShapeDtypeStruct((rows, cols), F32),
        in_specs=[VMEM] * (len(flat) + 2),
        out_specs=VMEM,
        scratch_shapes=dot_scratch(2 * len(pairs), rows, cols),
        input_output_aliases={len(flat) + 1: 0},
        compiler_params=params(24),
        cost_estimate=cost(4 * rows * cols * cols * len(pairs), 12 * rows * cols),
        name="dots",
    )(*flat, dense, prior)


def means_kernel(n_pairs, s_rows, order, *refs):
    msgs, (thr_ref, panel_ref, out_ref, flag_ref) = refs[:n_pairs], refs[n_pairs:]
    _, z, core = place()
    cols = panel_ref.shape[1]
    tj = cols // TB
    total = jnp.zeros((8, cols), F32)
    row = lax.broadcasted_iota(I32, (8, TB), 0)
    over = jnp.zeros((1, TB), F32)
    for q in range(n_pairs):
        for b in range(2):
            over = jnp.maximum(over, msgs[q][b * s_rows + tj : b * s_rows + tj + 1, :])
            for t in range(tj):
                s = jnp.broadcast_to(msgs[q][b * s_rows + t : b * s_rows + t + 1, :], (8, TB))
                high = s.astype(BF16).astype(F32)
                mid = (s - high).astype(BF16).astype(F32)
                low = s - high - mid
                lhs = jnp.where(row == 0, high, jnp.where(row == 1, mid, jnp.where(row == 2, low, 0.0)))
                at = (z ^ q) * 2 * cols + (core ^ b) * cols + t * TB
                total += jnp.dot(
                    lhs.astype(BF16),
                    panel_ref[pl.ds(pl.multiple_of(at, TB), TB), :],
                    preferred_element_type=F32,
                )
    mean = jnp.sum(total, axis=0, keepdims=True) / order
    out_ref[...] = jnp.broadcast_to(0.125 * thr_ref[...].astype(F32) * mean, out_ref.shape)
    flag_ref[0] = jnp.where(jnp.max(over) > 0.0, 1, 0).astype(I32)


def cuts_of(messages, thr, dense, s_rows, order):
    n = len(messages)
    cols = dense.shape[1]
    return pl.pallas_call(
        functools.partial(means_kernel, n, s_rows, order),
        out_shape=(jax.ShapeDtypeStruct((8, cols), F32), jax.ShapeDtypeStruct((1,), I32)),
        in_specs=[VMEM] * (n + 2),
        out_specs=(VMEM, SMEM),
        compiler_params=params(12),
        cost_estimate=cost(1e7, dense.size * 2),
        name="cuts",
    )(*messages, thr, dense)


def last_kernel(pair, rows, *refs):
    blocks, (panel_ref, prior_ref, cut_ref, keep_ref, acc_ref, tot_ref) = refs[:4], refs[4:10]
    itab, stab, sem, lhs = refs[10:]
    step = strip_rows(rows)
    cols = panel_ref.shape[1]
    per = step // TB
    totals = [jnp.zeros((8, cols), F32)]
    read_tables(blocks[:2], itab, stab, sem)

    def use(m, got):
        prior = prior_ref[m * step : (m + 1) * step, :]
        got = jnp.maximum((prior if got is None else prior + got) - cut_ref[0:1, :], 0.0)
        for a in range(per):
            i = m * per + a
            cell = got[a * TB : (a + 1) * TB, :] * keep_ref[i : i + 1, :]
            acc_ref[i * TB : (i + 1) * TB, :] = cell
            totals[0] += jnp.sum(cell.reshape(TB // 8, 8, cols), axis=0)

    products("pools", blocks, pair, panel_ref, stab, (0, 1), lhs, rows, use)
    tot_ref[...] = jnp.sum(totals[0], axis=0, keepdims=True)


def finish(keep, blocks, pair, dense, prior, cut, rows):
    cols = dense.shape[1]
    return pl.pallas_call(
        functools.partial(last_kernel, pair, rows),
        out_shape=(jax.ShapeDtypeStruct((rows, cols), F32), jax.ShapeDtypeStruct((1, cols), F32)),
        in_specs=[VMEM] * 8,
        out_specs=(VMEM, VMEM),
        scratch_shapes=dot_scratch(2, rows, cols),
        compiler_params=params(20),
        cost_estimate=cost(4 * rows * cols * cols, 12 * rows * cols),
        name="finish",
    )(*blocks, dense, prior, cut, keep)


def scale_kernel(n, order, x_ref, *refs):
    tots, out_ref = refs[:n], refs[n]
    total = tots[0][...]
    for t in tots[1:]:
        total = total + t[...]
    total = total / order
    factor = 1.0 / jnp.maximum(total, 0.1)
    out_ref[...] = (x_ref[...] * factor).astype(BF16)


def scale(x, totals, order):
    n = len(totals)
    return pl.pallas_call(
        functools.partial(scale_kernel, n, order),
        out_shape=jax.ShapeDtypeStruct(x.shape, BF16),
        in_specs=[VMEM] * (n + 1),
        out_specs=VMEM,
        compiler_params=params(12),
        cost_estimate=cost(2 * x.size, 6 * x.size),
        name="scale",
    )(x, *totals)


def dense_path(values, tile_mask, keep_mask, thr_index, n_row, n_col):
    rows, cols = values.shape
    ti, tj = tiles_of(values.shape)
    matrix = (
        values.reshape(ti, TB, tj, TB) * tile_mask[:, None, :, None].astype(BF16)
    ).reshape(rows, cols)
    kept = jnp.broadcast_to(keep_mask[:, None, :, None].astype(F32), (ti, TB, tj, TB)).reshape(rows, cols)
    r, c = lax.axis_index("row"), lax.axis_index("col")
    order = rows * n_row

    def col_ring(i, carry):
        block, panel_ = carry
        panel_ = lax.dynamic_update_slice(panel_, block, (((r - i) % n_row) * rows, 0))
        return lax.ppermute(block, "row", [(k, (k + 1) % n_row) for k in range(n_row)]), panel_

    _, panel_ = lax.fori_loop(0, n_row, col_ring, (matrix, jnp.zeros((order, cols), BF16)))

    def row_ring(i, carry):
        block, acc = carry
        part = lax.dynamic_slice(panel_, (((c - i) % n_col) * cols, 0), (cols, cols))
        acc = acc + jnp.dot(block, part, preferred_element_type=F32)
        return lax.ppermute(block, "col", [(k, (k + 1) % n_col) for k in range(n_col)]), acc

    _, product = lax.fori_loop(0, n_col, row_ring, (matrix, jnp.zeros((rows, cols), F32)))
    means = lax.psum(jnp.sum(product, axis=0), "row") / order
    pruned = jnp.maximum(product - 0.125 * thr_index.astype(F32) * means, 0.0) * kept
    totals = lax.psum(jnp.sum(pruned, axis=0), "row") / order
    return (pruned / jnp.maximum(totals, 0.1)).astype(BF16)


def on_device(values, tile_mask, keep_mask, thr_index, n_row, n_col):
    return body(values, tile_mask, keep_mask, thr_index, n_row, n_col)


def body(values, tile_mask, keep_mask, thr_index, n_row, n_col):
    rows, cols = values.shape
    ti, tj = tiles_of(values.shape)
    first = ti * tj // 2
    extra = ti * tj * 3 // 16
    slots = ti * tj * 13 // 16
    n_z = n_col // 2
    last = n_z - 1
    order = rows * n_row

    def send(x, dr=0, dz=0, dc=0):
        pairs = [
            (r * n_col + z * 2 + c, (r ^ dr) * n_col + (z ^ dz) * 2 + (c ^ dc))
            for r in range(n_row)
            for z in range(n_z)
            for c in range(2)
        ]
        return lax.ppermute(x, AXES, pairs)

    own = pack(values, tile_mask.T, slots, first)
    own_swapped = [send(x, dc=1) for x in own]
    spare, sums = pool(values, tile_mask.T, own[1], own_swapped[1], first, extra)

    line = {0: [own[0], spare]}
    swapped = {}
    for j in range(1, n_z):
        low = j & -j
        line[j] = [send(x, dz=low) for x in line[j ^ low]]
        swapped[j] = [send(x, dc=1) for x in line[j]]

    column = {0: own}
    for q in range(1, n_row):
        low = q & -q
        rest = q ^ low
        if rest and rest & -rest == rest:
            column[q] = [send(column[low][0], dr=rest), send(column[rest][1], dr=low)]
        else:
            column[q] = [send(x, dr=q) for x in own]

    dense, acc = panel([column[q] for q in range(n_row)], own_swapped, rows, cols)

    sums = functools.reduce(jnp.add, [send(sums, dr=q) for q in range(1, n_row)], sums)
    both = jnp.concatenate([sums, send(sums, dc=1)], axis=0)
    messages = [both] + [send(both, dz=j) for j in range(1, n_z)]
    cut, over = cuts_of(messages, thr_index.reshape(1, cols), dense, sums.shape[0], order)

    early = tuple(range(1, last))
    if early:
        blocks = [(line[j][0], swapped[j][0], line[j][1], swapped[j][1]) for j in early]
        acc = dots("all", blocks, early, dense, acc, rows)
    acc = dots("heads", [(line[last][0], swapped[last][0])], (last,), dense, acc, rows)
    keep = jnp.repeat(keep_mask.astype(F32), TB, axis=1)

    def fast():
        blocks = (line[last][0], swapped[last][0], line[last][1], swapped[last][1])
        pruned, tot = finish(keep, blocks, last, dense, acc, cut, rows)
        totals = {0: tot}
        for q in range(1, n_row):
            low = q & -q
            totals[q] = send(totals[q ^ low], dr=low)
        totals = list(totals.values())
        return scale(pruned, totals, order)

    def full():
        return dense_path(values, tile_mask, keep_mask, thr_index, n_row, n_col)

    return lax.cond(over[0] > 0, full, fast)


def solution(mesh):
    n_row, n_col = mesh.shape["row"], mesh.shape["col"]
    return jax.shard_map(
        functools.partial(on_device, n_row=n_row, n_col=n_col),
        mesh=mesh,
        in_specs=(P("row", "col"), P("row", "col"), P("row", "col"), P("col")),
        out_specs=P("row", "col"),
        check_vma=False,
    )
```

```python
import functools

import jax
import jax.numpy as jnp
from jax import lax
from jax.experimental import pallas as pl
from jax.experimental.pallas import tpu as pltpu
from jax.sharding import PartitionSpec as P

TB = 128
PAD = 16
AXES = ("row", "col")
F32, BF16, I32 = jnp.float32, jnp.bfloat16, jnp.int32
VMEM = pl.BlockSpec(memory_space=pltpu.VMEM)
SMEM = pl.BlockSpec(memory_space=pltpu.SMEM)


def params(mib):
    return pltpu.CompilerParams(vmem_limit_bytes=mib * 1024 * 1024)


def cost(flops, moved):
    return pl.CostEstimate(flops=int(flops), bytes_accessed=int(moved), transcendentals=0)


def tiles_of(shape):
    return shape[0] // TB, shape[1] // TB


def place():
    col = lax.axis_index("col")
    return lax.axis_index("row"), col // 2, col % 2


def table_of(ref):
    end = ref.shape[0]
    return ref[end - PAD : end, :].astype(F32).astype(I32)[0:1, :]


def places(ref):
    return (ref.shape[0] - PAD) // TB


def pack_kernel(mask_in, block_in, head_ref, rest_ref, mask_ref, block_ref, mask_sem, sems):
    ti, tj = tiles_of(block_ref.shape)
    get_mask = pltpu.make_async_copy(mask_in, mask_ref, mask_sem)
    get_mask.start()
    chunk = block_ref.shape[0] // sems.shape[0]
    gets = []
    for k in range(sems.shape[0]):
        here = pl.ds(k * chunk, chunk)
        gets.append(pltpu.make_async_copy(block_in.at[here, :], block_ref.at[here, :], sems.at[k]))
        gets[-1].start()
    get_mask.wait()
    first, slots = places(head_ref), places(head_ref) + places(rest_ref)
    lane = lax.broadcasted_iota(I32, (PAD, TB), 1)
    table = jnp.full((PAD, TB), -1, I32)
    used = jnp.int32(0)
    for i in range(ti):
        if i * TB % chunk == 0:
            gets[i * TB // chunk].wait()
        for j in range(tj):
            stored = mask_ref[j, i]

            @pl.when(jnp.logical_and(stored > 0, used < first))
            def _(i=i, j=j, used=used):
                tile = block_ref[i * TB : (i + 1) * TB, j * TB : (j + 1) * TB]
                head_ref[pl.ds(pl.multiple_of(used * TB, TB), TB), :] = tile

            if i * tj + j >= first:

                @pl.when(jnp.logical_and(stored > 0, jnp.logical_and(used >= first, used < slots)))
                def _(i=i, j=j, used=used):
                    tile = block_ref[i * TB : (i + 1) * TB, j * TB : (j + 1) * TB]
                    rest_ref[pl.ds(pl.multiple_of((used - first) * TB, TB), TB), :] = tile

            table = jnp.where(lane == i * tj + j, jnp.where(stored > 0, used, -1), table)
            used = used + stored
    table = jnp.where(lane == ti * tj, used, table).astype(F32).astype(BF16)
    head_ref[first * TB :, :] = table
    rest_ref[(slots - first) * TB :, :] = table


def pack(block, mask_t, slots, first):
    return pl.pallas_call(
        pack_kernel,
        out_shape=tuple(jax.ShapeDtypeStruct((n * TB + PAD, TB), BF16) for n in (first, slots - first)),
        in_specs=[pl.BlockSpec(memory_space=pl.ANY)] * 2,
        out_specs=(VMEM, VMEM),
        scratch_shapes=[
            pltpu.SMEM(mask_t.shape, I32),
            pltpu.VMEM(block.shape, BF16),
            pltpu.SemaphoreType.DMA,
            pltpu.SemaphoreType.DMA((2,)),
        ],
        compiler_params=params(8),
        cost_estimate=cost(1e6, 2 * block.size * 2),
        name="pack",
    )(mask_t, block)


def load(ref, at, count):
    return ref[pl.ds(pl.multiple_of(jnp.clip(at, 0, count - 1) * TB, TB), TB), :]


def pool_kernel(first, mask_ref, block_ref, rest_ref, other_ref, out_ref, msg_ref):
    ti, tj = tiles_of(block_ref.shape)
    spare, n = places(rest_ref), out_ref.shape[0] // TB
    core = place()[2]
    count = jnp.int32(0)
    sums = [jnp.zeros((8, TB), F32) for _ in range(tj)]
    for i in range(ti):
        for j in range(tj):
            stored = mask_ref[j, i]
            count = count + stored
            tile = block_ref[i * TB : (i + 1) * TB, j * TB : (j + 1) * TB].astype(F32)
            sums[j] += jnp.sum(tile.reshape(TB // 8, 8, TB), axis=0) * stored.astype(F32)
    lane = lax.broadcasted_iota(I32, (1, TB), 1)
    theirs = jnp.max(jnp.where(lane == ti * tj, table_of(other_ref), 0))
    left = jnp.maximum(count - first, 0)
    left_other = jnp.maximum(theirs - first, 0)
    left_0 = jnp.where(core == 0, left, left_other)
    for i in range(n):
        p = core * n + i
        in_0 = p < left_0
        at = jnp.where(in_0, p, p - left_0)
        mine = jnp.where(in_0, 0, 1) == core
        tile = jnp.where(mine, load(rest_ref, at, spare), load(other_ref, at, spare))
        out_ref[i * TB : (i + 1) * TB, :] = tile
    over = jnp.logical_or(left > spare, left + left_other > 2 * n)
    msg_ref[...] = jnp.zeros_like(msg_ref)
    for j in range(tj):
        msg_ref[j : j + 1, :] = jnp.sum(sums[j], axis=0, keepdims=True)
    msg_ref[tj : tj + 1, :] = jnp.full((1, TB), 1.0, F32) * jnp.where(over, 1.0, 0.0)


def pool(block, mask_t, rest, other, first, n):
    s_rows = -(-(block.shape[1] // TB + 1) // 8) * 8
    return pl.pallas_call(
        functools.partial(pool_kernel, first),
        out_shape=(
            jax.ShapeDtypeStruct((n * TB, TB), BF16),
            jax.ShapeDtypeStruct((s_rows, TB), F32),
        ),
        in_specs=[SMEM] + [VMEM] * 3,
        out_specs=(VMEM, VMEM),
        compiler_params=params(8),
        cost_estimate=cost(1e6, 2 * block.size * 2),
        name="pool",
    )(mask_t, block, rest, other)


def start_tables(refs, itab, stab, sem):
    for q, ref in enumerate(refs):
        itab[q : q + 1, :] = table_of(ref)
    copy = pltpu.make_async_copy(itab, stab, sem)
    copy.start()
    return copy


def read_tables(refs, itab, stab, sem):
    start_tables(refs, itab, stab, sem).wait()


def zero_tile():
    return jnp.zeros((TB, TB), BF16)


def whole_tile(parts, at, low):
    first = places(parts[0])
    tile = load(parts[0], at, first)
    if not low:
        tile = jnp.where(at >= first, load(parts[1], at - first, places(parts[1])), tile)
    return jnp.where(at >= 0, tile, zero_tile())


def table_scratch(n):
    n8 = -(-n // 8) * 8
    return [pltpu.VMEM((n8, TB), I32), pltpu.SMEM((n8, TB), I32), pltpu.SemaphoreType.DMA]


def regroup(refs, sizes):
    out = []
    for s in sizes:
        out.append(refs[:s])
        refs = refs[s:]
    return out


def strip_rows(rows):
    return min(rows, 256)


def tile_getters(kind, refs, stab, at_table, tiles, core):
    first = places(refs[0])
    if kind == "whole":
        return [lambda at, low, b=b: whole_tile((refs[b], refs[2 + b]), at, low) for b in range(2)]

    def head(side, at):
        return jnp.where(
            jnp.logical_and(at >= 0, at < first), load(refs[side], at, first), zero_tile()
        )

    if kind == "heads":
        return [lambda at, low, b=b: head(b, at) for b in range(len(refs))]
    n = refs[2].shape[0] // TB
    left = [jnp.maximum(stab[at_table[b], tiles] - first, 0) for b in range(2)]
    left_0 = jnp.where(core == 0, left[0], left[1])

    def getter(side):
        base = jnp.where((core ^ side) == 1, left_0, 0) - first

        def get(at, low):
            if low:
                return head(side, at)
            p = at + base
            part = jnp.where(p >= n, 1, 0)
            local = p - part * n
            rest = jnp.where(part == core, load(refs[2], local, n), load(refs[3], local, n))
            if kind == "pools":
                return jnp.where(at >= first, rest, zero_tile())
            return jnp.where(at >= first, rest, head(side, at))

        return get

    return [getter(0), getter(1)]


def products(kind, refs, pair, panel_ref, stab, at_table, lhs, rows, use, sides=(0, 1), tables=None):
    cols = panel_ref.shape[1]
    step = strip_rows(rows)
    tj = cols // TB
    _, z, core = place()
    n = rows // step
    safe = places(refs[0]) // tj
    start = safe * TB // step if kind == "pools" else 0
    for m in range(start):
        use(m, None)
    if tables is not None:
        tables.wait()
    getters = tile_getters(kind, refs, stab, at_table, rows // TB * tj, core)

    def unpack(m):
        for b, get in enumerate(getters):
            for a in range(step // TB):
                i = m * (step // TB) + a
                tiles = [get(stab[at_table[b], i * tj + j], i < safe) for j in range(tj)]
                lhs[m % 2, a * TB : (a + 1) * TB, b * cols : (b + 1) * cols] = jnp.concatenate(tiles, axis=1)

    unpack(start)
    for m in range(start, n):
        if m + 1 < n:
            unpack(m + 1)
        total = None
        for b, side in enumerate(sides):
            at = pl.multiple_of((z ^ pair) * 2 * cols + (core ^ side) * cols, TB)
            got = jnp.dot(
                lhs[m % 2, :, b * cols : (b + 1) * cols],
                panel_ref[pl.ds(at, cols), :],
                preferred_element_type=F32,
            )
            total = got if total is None else total + got
        use(m, total)


def adder(acc_ref, prior_ref, rows):
    step = strip_rows(rows)

    def use(m, got):
        here = slice(m * step, (m + 1) * step)
        acc_ref[here, :] = got if prior_ref is None else prior_ref[here, :] + got

    return use


def dot_scratch(n, rows, cols):
    return table_scratch(n) + [pltpu.VMEM((2, strip_rows(rows), 2 * cols), BF16)]


def panel_kernel(n, rows, *refs):
    blocks, other = regroup(refs, [2] * n), refs[2 * n : 2 * n + 2]
    panel_ref, acc_ref, itab, stab, sem, lhs = refs[2 * n + 2 :]
    cols = panel_ref.shape[1]
    ti, tj = rows // TB, cols // TB
    me = place()[0]
    read_tables([b[1] for b in blocks] + [other[1]], itab, stab, sem)
    safe = places(blocks[0][0]) // tj
    for q in range(n):
        base = (me ^ q) * rows

        def strip(i, done, q=q, base=base, low=False):
            tiles = [whole_tile(blocks[q], stab[q, i * tj + j], low) for j in range(tj)]
            panel_ref[pl.ds(pl.multiple_of(base + i * TB, TB), TB), :] = jnp.concatenate(tiles, axis=1)
            return done

        lax.fori_loop(0, safe, functools.partial(strip, low=True), 0, unroll=2)
        lax.fori_loop(safe, ti, strip, 0, unroll=2)
    mine = blocks[0]
    heads_rests = (mine[0], other[0], mine[1], other[1])
    products("whole", heads_rests, 0, panel_ref, stab, (0, n), lhs, rows, adder(acc_ref, None, rows))


def panel(payloads, other, rows, cols):
    n = len(payloads)
    return pl.pallas_call(
        functools.partial(panel_kernel, n, rows),
        out_shape=(
            jax.ShapeDtypeStruct((n * rows, cols), BF16),
            jax.ShapeDtypeStruct((rows, cols), F32),
        ),
        in_specs=[VMEM] * (2 * n + 2),
        out_specs=(VMEM, VMEM),
        scratch_shapes=dot_scratch(n + 1, rows, cols),
        compiler_params=params(24),
        cost_estimate=cost(4 * rows * cols * cols, 2 * n * rows * cols * 2),
        name="panel",
    )(*[x for p in payloads for x in p], *other)


def dot_kernel(kind, pairs, rows, *refs):
    blocks = regroup(refs, [4] * len(pairs))
    panel_ref, prior_ref, acc_ref, itab, stab, sem, lhs = refs[4 * len(pairs) :]
    read_tables([r for b in blocks for r in b[:2]], itab, stab, sem)
    for k, (pair, b) in enumerate(zip(pairs, blocks)):
        use = adder(acc_ref, acc_ref if k else prior_ref, rows)
        products(kind, b, pair, panel_ref, stab, (2 * k, 2 * k + 1), lhs, rows, use)


def head_kernel(side, pair, rows, head_ref, panel_ref, prior_ref, acc_ref, itab, stab, sem, lhs):
    read_tables([head_ref], itab, stab, sem)
    use = adder(acc_ref, prior_ref, rows)
    products("heads", [head_ref], pair, panel_ref, stab, (0,), lhs, rows, use, sides=(side,))


def add_products(kernel, payloads, dense, prior, rows, n_tables):
    cols = dense.shape[1]
    return pl.pallas_call(
        kernel,
        out_shape=jax.ShapeDtypeStruct((rows, cols), F32),
        in_specs=[VMEM] * (len(payloads) + 2),
        out_specs=VMEM,
        scratch_shapes=dot_scratch(n_tables, rows, cols),
        input_output_aliases={len(payloads) + 1: 0},
        compiler_params=params(24),
        cost_estimate=cost(2 * rows * cols * cols * n_tables, 12 * rows * cols),
        name="dots",
    )(*payloads, dense, prior)


def dots(blocks, pairs, dense, prior, rows):
    kernel = functools.partial(dot_kernel, "all", pairs, rows)
    return add_products(kernel, [x for b in blocks for x in b], dense, prior, rows, 2 * len(pairs))


def head_dots(head, side, pair, dense, prior, rows):
    kernel = functools.partial(head_kernel, side, pair, rows)
    return add_products(kernel, [head], dense, prior, rows, 1)


def total_kernel(*refs):
    refs[-1][...] = functools.reduce(jnp.add, [r[...] for r in refs[:-1]])


def total_of(xs):
    return pl.pallas_call(
        total_kernel,
        out_shape=jax.ShapeDtypeStruct(xs[0].shape, F32),
        in_specs=[VMEM] * len(xs),
        out_specs=VMEM,
        compiler_params=params(4),
        cost_estimate=cost(1e5, 4 * xs[0].size * len(xs)),
        name="total",
    )(*xs)


def means_kernel(n_pairs, s_rows, order, *refs):
    msgs, (thr_ref, panel_ref, out_ref, flag_ref) = refs[:n_pairs], refs[n_pairs:]
    _, z, core = place()
    cols = panel_ref.shape[1]
    tj = cols // TB
    total = jnp.zeros((8, cols), F32)
    row = lax.broadcasted_iota(I32, (8, TB), 0)
    over = jnp.zeros((1, TB), F32)
    for q in range(n_pairs):
        for b in range(2):
            over = jnp.maximum(over, msgs[q][b * s_rows + tj : b * s_rows + tj + 1, :])
            for t in range(tj):
                s = jnp.broadcast_to(msgs[q][b * s_rows + t : b * s_rows + t + 1, :], (8, TB))
                high = s.astype(BF16).astype(F32)
                mid = (s - high).astype(BF16).astype(F32)
                low = s - high - mid
                lhs = jnp.where(row == 0, high, jnp.where(row == 1, mid, jnp.where(row == 2, low, 0.0)))
                at = (z ^ q) * 2 * cols + (core ^ b) * cols + t * TB
                total += jnp.dot(
                    lhs.astype(BF16),
                    panel_ref[pl.ds(pl.multiple_of(at, TB), TB), :],
                    preferred_element_type=F32,
                )
    mean = jnp.sum(total, axis=0, keepdims=True) / order
    out_ref[...] = jnp.broadcast_to(0.125 * thr_ref[...].astype(F32) * mean, out_ref.shape)
    flag_ref[0] = jnp.where(jnp.max(over) > 0.0, 1, 0).astype(I32)


def cuts_of(messages, thr, dense, s_rows, order):
    n = len(messages)
    cols = dense.shape[1]
    return pl.pallas_call(
        functools.partial(means_kernel, n, s_rows, order),
        out_shape=(jax.ShapeDtypeStruct((8, cols), F32), jax.ShapeDtypeStruct((1,), I32)),
        in_specs=[VMEM] * (n + 2),
        out_specs=(VMEM, SMEM),
        compiler_params=params(12),
        cost_estimate=cost(1e7, dense.size * 2),
        name="cuts",
    )(*messages, thr, dense)


def last_kernel(pair, rows, *refs):
    blocks, (panel_ref, prior_ref, cut_ref, keep_ref, acc_ref, tot_ref) = refs[:4], refs[4:10]
    itab, stab, sem, lhs = refs[10:]
    step = strip_rows(rows)
    cols = panel_ref.shape[1]
    per = step // TB
    totals = [jnp.zeros((8, cols), F32)]
    tables = start_tables(blocks[:2], itab, stab, sem)

    def use(m, got):
        prior = prior_ref[m * step : (m + 1) * step, :]
        got = jnp.maximum((prior if got is None else prior + got) - cut_ref[0:1, :], 0.0)
        for a in range(per):
            i = m * per + a
            cell = got[a * TB : (a + 1) * TB, :] * keep_ref[i : i + 1, :]
            acc_ref[i * TB : (i + 1) * TB, :] = cell
            totals[0] += jnp.sum(cell.reshape(TB // 8, 8, cols), axis=0)

    products("pools", blocks, pair, panel_ref, stab, (0, 1), lhs, rows, use, tables=tables)
    tot_ref[...] = jnp.sum(totals[0], axis=0, keepdims=True)


def finish(keep, blocks, pair, dense, prior, cut, rows):
    cols = dense.shape[1]
    return pl.pallas_call(
        functools.partial(last_kernel, pair, rows),
        out_shape=(jax.ShapeDtypeStruct((rows, cols), F32), jax.ShapeDtypeStruct((1, cols), F32)),
        in_specs=[VMEM] * 8,
        out_specs=(VMEM, VMEM),
        scratch_shapes=dot_scratch(2, rows, cols),
        compiler_params=params(20),
        cost_estimate=cost(4 * rows * cols * cols, 12 * rows * cols),
        name="finish",
    )(*blocks, dense, prior, cut, keep)


def scale_kernel(n, order, x_ref, *refs):
    tots, out_ref = refs[:n], refs[n]
    total = tots[0][...]
    for t in tots[1:]:
        total = total + t[...]
    total = total / order
    factor = 1.0 / jnp.maximum(total, 0.1)
    out_ref[...] = (x_ref[...] * factor).astype(BF16)


def scale(x, totals, order):
    n = len(totals)
    return pl.pallas_call(
        functools.partial(scale_kernel, n, order),
        out_shape=jax.ShapeDtypeStruct(x.shape, BF16),
        in_specs=[VMEM] * (n + 1),
        out_specs=VMEM,
        compiler_params=params(12),
        cost_estimate=cost(2 * x.size, 6 * x.size),
        name="scale",
    )(x, *totals)


def dense_path(values, tile_mask, keep_mask, thr_index, n_row, n_col):
    rows, cols = values.shape
    ti, tj = tiles_of(values.shape)
    matrix = (
        values.reshape(ti, TB, tj, TB) * tile_mask[:, None, :, None].astype(BF16)
    ).reshape(rows, cols)
    kept = jnp.broadcast_to(keep_mask[:, None, :, None].astype(F32), (ti, TB, tj, TB)).reshape(rows, cols)
    r, c = lax.axis_index("row"), lax.axis_index("col")
    order = rows * n_row

    def col_ring(i, carry):
        block, panel_ = carry
        panel_ = lax.dynamic_update_slice(panel_, block, (((r - i) % n_row) * rows, 0))
        return lax.ppermute(block, "row", [(k, (k + 1) % n_row) for k in range(n_row)]), panel_

    _, panel_ = lax.fori_loop(0, n_row, col_ring, (matrix, jnp.zeros((order, cols), BF16)))

    def row_ring(i, carry):
        block, acc = carry
        part = lax.dynamic_slice(panel_, (((c - i) % n_col) * cols, 0), (cols, cols))
        acc = acc + jnp.dot(block, part, preferred_element_type=F32)
        return lax.ppermute(block, "col", [(k, (k + 1) % n_col) for k in range(n_col)]), acc

    _, product = lax.fori_loop(0, n_col, row_ring, (matrix, jnp.zeros((rows, cols), F32)))
    means = lax.psum(jnp.sum(product, axis=0), "row") / order
    pruned = jnp.maximum(product - 0.125 * thr_index.astype(F32) * means, 0.0) * kept
    totals = lax.psum(jnp.sum(pruned, axis=0), "row") / order
    return (pruned / jnp.maximum(totals, 0.1)).astype(BF16)


def on_device(values, tile_mask, keep_mask, thr_index, n_row, n_col):
    return body(values, tile_mask, keep_mask, thr_index, n_row, n_col)


def body(values, tile_mask, keep_mask, thr_index, n_row, n_col):
    rows, cols = values.shape
    ti, tj = tiles_of(values.shape)
    first = ti * tj // 2
    extra = ti * tj * 3 // 16
    slots = ti * tj * 13 // 16
    n_z = n_col // 2
    last = n_z - 1
    order = rows * n_row

    def send(x, dr=0, dz=0, dc=0):
        pairs = [
            (r * n_col + z * 2 + c, (r ^ dr) * n_col + (z ^ dz) * 2 + (c ^ dc))
            for r in range(n_row)
            for z in range(n_z)
            for c in range(2)
        ]
        return lax.ppermute(x, AXES, pairs)

    own = pack(values, tile_mask.T, slots, first)
    own_swapped = [send(x, dc=1) for x in own]
    spare, sums = pool(values, tile_mask.T, own[1], own_swapped[1], first, extra)

    line = {0: [own[0], spare]}
    swapped = {}
    for j in range(1, n_z):
        low = j & -j
        line[j] = [send(x, dz=low) for x in line[j ^ low]]
        swapped[j] = [send(x, dc=1) for x in line[j]]

    column = {0: own}
    for q in range(1, n_row):
        low = q & -q
        rest = q ^ low
        if rest and rest & -rest == rest:
            column[q] = [send(column[low][0], dr=rest), send(column[rest][1], dr=low)]
        else:
            column[q] = [send(x, dr=q) for x in own]

    dense, acc = panel([column[q] for q in range(n_row)], own_swapped, rows, cols)

    sums = [sums] + [send(sums, dr=q) for q in range(1, n_row)]
    sums = total_of(sums)
    both = jnp.concatenate([sums, send(sums, dc=1)], axis=0)
    messages = [both] + [send(both, dz=j) for j in range(1, n_z)]
    cut, over = cuts_of(messages, thr_index.reshape(1, cols), dense, sums.shape[0], order)

    early = tuple(range(1, last))
    if early:
        blocks = [(line[j][0], swapped[j][0], line[j][1], swapped[j][1]) for j in early]
        acc = dots(blocks, early, dense, acc, rows)
    acc = head_dots(line[last][0], 0, last, dense, acc, rows)
    acc = head_dots(swapped[last][0], 1, last, dense, acc, rows)
    keep = jnp.repeat(keep_mask.astype(F32), TB, axis=1)

    def fast():
        blocks = (line[last][0], swapped[last][0], line[last][1], swapped[last][1])
        pruned, tot = finish(keep, blocks, last, dense, acc, cut, rows)
        totals = {0: tot}
        for q in range(1, n_row):
            low = q & -q
            totals[q] = send(totals[q ^ low], dr=low)
        totals = list(totals.values())
        return scale(pruned, totals, order)

    def full():
        return dense_path(values, tile_mask, keep_mask, thr_index, n_row, n_col)

    return lax.cond(over[0] > 0, full, fast)


def solution(mesh):
    n_row, n_col = mesh.shape["row"], mesh.shape["col"]
    return jax.shard_map(
        functools.partial(on_device, n_row=n_row, n_col=n_col),
        mesh=mesh,
        in_specs=(P("row", "col"), P("row", "col"), P("row", "col"), P("col")),
        out_specs=P("row", "col"),
        check_vma=False,
    )
```

```python
import functools

import jax
import jax.numpy as jnp
from jax import lax
from jax.experimental import pallas as pl
from jax.experimental.pallas import tpu as pltpu
from jax.sharding import PartitionSpec as P

TB = 128
PAD = 16
AXES = ("row", "col")
F32, BF16, I32 = jnp.float32, jnp.bfloat16, jnp.int32
VMEM = pl.BlockSpec(memory_space=pltpu.VMEM)
SMEM = pl.BlockSpec(memory_space=pltpu.SMEM)


def params(mib):
    return pltpu.CompilerParams(vmem_limit_bytes=mib * 1024 * 1024)


def cost(flops, moved):
    return pl.CostEstimate(flops=int(flops), bytes_accessed=int(moved), transcendentals=0)


def tiles_of(shape):
    return shape[0] // TB, shape[1] // TB


def place():
    col = lax.axis_index("col")
    return lax.axis_index("row"), col // 2, col % 2


def table_of(ref):
    end = ref.shape[0]
    return ref[end - PAD : end, :].astype(F32).astype(I32)[0:1, :]


def places(ref):
    return (ref.shape[0] - PAD) // TB


def pack_kernel(mask_in, block_in, head_ref, rest_ref, mask_ref, block_ref, mask_sem, sems):
    ti, tj = tiles_of(block_ref.shape)
    get_mask = pltpu.make_async_copy(mask_in, mask_ref, mask_sem)
    get_mask.start()
    chunk = block_ref.shape[0] // sems.shape[0]
    gets = []
    for k in range(sems.shape[0]):
        here = pl.ds(k * chunk, chunk)
        gets.append(pltpu.make_async_copy(block_in.at[here, :], block_ref.at[here, :], sems.at[k]))
        gets[-1].start()
    get_mask.wait()
    first, slots = places(head_ref), places(head_ref) + places(rest_ref)
    lane = lax.broadcasted_iota(I32, (PAD, TB), 1)
    table = jnp.full((PAD, TB), -1, I32)
    used = jnp.int32(0)
    for i in range(ti):
        if i * TB % chunk == 0:
            gets[i * TB // chunk].wait()
        for j in range(tj):
            stored = mask_ref[j, i]

            @pl.when(jnp.logical_and(stored > 0, used < first))
            def _(i=i, j=j, used=used):
                tile = block_ref[i * TB : (i + 1) * TB, j * TB : (j + 1) * TB]
                head_ref[pl.ds(pl.multiple_of(used * TB, TB), TB), :] = tile

            if i * tj + j >= first:

                @pl.when(jnp.logical_and(stored > 0, jnp.logical_and(used >= first, used < slots)))
                def _(i=i, j=j, used=used):
                    tile = block_ref[i * TB : (i + 1) * TB, j * TB : (j + 1) * TB]
                    rest_ref[pl.ds(pl.multiple_of((used - first) * TB, TB), TB), :] = tile

            table = jnp.where(lane == i * tj + j, jnp.where(stored > 0, used, -1), table)
            used = used + stored
    table = jnp.where(lane == ti * tj, used, table).astype(F32).astype(BF16)
    head_ref[first * TB :, :] = table
    rest_ref[(slots - first) * TB :, :] = table


def pack(block, mask_t, slots, first):
    return pl.pallas_call(
        pack_kernel,
        out_shape=tuple(jax.ShapeDtypeStruct((n * TB + PAD, TB), BF16) for n in (first, slots - first)),
        in_specs=[pl.BlockSpec(memory_space=pl.ANY)] * 2,
        out_specs=(VMEM, VMEM),
        scratch_shapes=[
            pltpu.SMEM(mask_t.shape, I32),
            pltpu.VMEM(block.shape, BF16),
            pltpu.SemaphoreType.DMA,
            pltpu.SemaphoreType.DMA((2,)),
        ],
        compiler_params=params(8),
        cost_estimate=cost(1e6, 2 * block.size * 2),
        name="pack",
    )(mask_t, block)


def load(ref, at, count):
    return ref[pl.ds(pl.multiple_of(jnp.clip(at, 0, count - 1) * TB, TB), TB), :]


def pool_kernel(first, mask_ref, block_ref, rest_ref, other_ref, out_ref, msg_ref):
    ti, tj = tiles_of(block_ref.shape)
    spare, n = places(rest_ref), out_ref.shape[0] // TB
    core = place()[2]
    count = jnp.int32(0)
    sums = [jnp.zeros((8, TB), F32) for _ in range(tj)]
    for i in range(ti):
        for j in range(tj):
            stored = mask_ref[j, i]
            count = count + stored
            tile = block_ref[i * TB : (i + 1) * TB, j * TB : (j + 1) * TB].astype(F32)
            sums[j] += jnp.sum(tile.reshape(TB // 8, 8, TB), axis=0) * stored.astype(F32)
    lane = lax.broadcasted_iota(I32, (1, TB), 1)
    theirs = jnp.max(jnp.where(lane == ti * tj, table_of(other_ref), 0))
    left = jnp.maximum(count - first, 0)
    left_other = jnp.maximum(theirs - first, 0)
    left_0 = jnp.where(core == 0, left, left_other)
    for i in range(n):
        p = core * n + i
        in_0 = p < left_0
        at = jnp.where(in_0, p, p - left_0)
        mine = jnp.where(in_0, 0, 1) == core
        tile = jnp.where(mine, load(rest_ref, at, spare), load(other_ref, at, spare))
        out_ref[i * TB : (i + 1) * TB, :] = tile
    over = jnp.logical_or(left > spare, left + left_other > 2 * n)
    msg_ref[...] = jnp.zeros_like(msg_ref)
    for j in range(tj):
        msg_ref[j : j + 1, :] = jnp.sum(sums[j], axis=0, keepdims=True)
    msg_ref[tj : tj + 1, :] = jnp.full((1, TB), 1.0, F32) * jnp.where(over, 1.0, 0.0)


def pool(block, mask_t, rest, other, first, n):
    s_rows = -(-(block.shape[1] // TB + 1) // 8) * 8
    return pl.pallas_call(
        functools.partial(pool_kernel, first),
        out_shape=(
            jax.ShapeDtypeStruct((n * TB, TB), BF16),
            jax.ShapeDtypeStruct((s_rows, TB), F32),
        ),
        in_specs=[SMEM] + [VMEM] * 3,
        out_specs=(VMEM, VMEM),
        compiler_params=params(8),
        cost_estimate=cost(1e6, 2 * block.size * 2),
        name="pool",
    )(mask_t, block, rest, other)


def start_tables(refs, itab, stab, sem):
    for q, ref in enumerate(refs):
        itab[q : q + 1, :] = table_of(ref)
    copy = pltpu.make_async_copy(itab, stab, sem)
    copy.start()
    return copy


def read_tables(refs, itab, stab, sem):
    start_tables(refs, itab, stab, sem).wait()


def zero_tile():
    return jnp.zeros((TB, TB), BF16)


def whole_tile(parts, at, low):
    first = places(parts[0])
    tile = load(parts[0], at, first)
    if not low:
        tile = jnp.where(at >= first, load(parts[1], at - first, places(parts[1])), tile)
    return jnp.where(at >= 0, tile, zero_tile())


def table_scratch(n):
    n8 = -(-n // 8) * 8
    return [pltpu.VMEM((n8, TB), I32), pltpu.SMEM((n8, TB), I32), pltpu.SemaphoreType.DMA]


def regroup(refs, sizes):
    out = []
    for s in sizes:
        out.append(refs[:s])
        refs = refs[s:]
    return out


def strip_rows(rows):
    return min(rows, 256)


def tile_getters(kind, refs, stab, at_table, tiles, core):
    first = places(refs[0])
    if kind == "whole":
        return [lambda at, low, b=b: whole_tile((refs[b], refs[2 + b]), at, low) for b in range(2)]

    def head(side, at):
        return jnp.where(
            jnp.logical_and(at >= 0, at < first), load(refs[side], at, first), zero_tile()
        )

    if kind == "heads":
        return [lambda at, low, b=b: head(b, at) for b in range(len(refs))]
    n = refs[2].shape[0] // TB
    left = [jnp.maximum(stab[at_table[b], tiles] - first, 0) for b in range(2)]
    left_0 = jnp.where(core == 0, left[0], left[1])

    def getter(side):
        base = jnp.where((core ^ side) == 1, left_0, 0) - first

        def get(at, low):
            if low:
                return head(side, at)
            p = at + base
            part = jnp.where(p >= n, 1, 0)
            local = p - part * n
            rest = jnp.where(part == core, load(refs[2], local, n), load(refs[3], local, n))
            if kind == "pools":
                return jnp.where(at >= first, rest, zero_tile())
            return jnp.where(at >= first, rest, head(side, at))

        return get

    return [getter(0), getter(1)]


def products(kind, refs, pair, panel_ref, stab, at_table, lhs, rows, use, sides=(0, 1), tables=None):
    cols = panel_ref.shape[1]
    step = strip_rows(rows)
    tj = cols // TB
    _, z, core = place()
    n = rows // step
    safe = places(refs[0]) // tj
    start = safe * TB // step if kind == "pools" else 0
    for m in range(start):
        use(m, None)
    if tables is not None:
        tables.wait()
    getters = tile_getters(kind, refs, stab, at_table, rows // TB * tj, core)

    def unpack(m):
        for b, get in enumerate(getters):
            for a in range(step // TB):
                i = m * (step // TB) + a
                tiles = [get(stab[at_table[b], i * tj + j], i < safe) for j in range(tj)]
                lhs[m % 2, a * TB : (a + 1) * TB, b * cols : (b + 1) * cols] = jnp.concatenate(tiles, axis=1)

    unpack(start)
    for m in range(start, n):
        if m + 1 < n:
            unpack(m + 1)
        total = None
        for b, side in enumerate(sides):
            at = pl.multiple_of((z ^ pair) * 2 * cols + (core ^ side) * cols, TB)
            got = jnp.dot(
                lhs[m % 2, :, b * cols : (b + 1) * cols],
                panel_ref[pl.ds(at, cols), :],
                preferred_element_type=F32,
            )
            total = got if total is None else total + got
        use(m, total)


def adder(acc_ref, prior_ref, rows):
    step = strip_rows(rows)

    def use(m, got):
        here = slice(m * step, (m + 1) * step)
        acc_ref[here, :] = got if prior_ref is None else prior_ref[here, :] + got

    return use


def dot_scratch(n, rows, cols):
    return table_scratch(n) + [pltpu.VMEM((2, strip_rows(rows), 2 * cols), BF16)]


def panel_kernel(n, rows, *refs):
    blocks, other = regroup(refs, [2] * n), refs[2 * n : 2 * n + 2]
    panel_ref, acc_ref, itab, stab, sem, lhs = refs[2 * n + 2 :]
    cols = panel_ref.shape[1]
    ti, tj = rows // TB, cols // TB
    me = place()[0]
    read_tables([b[1] for b in blocks] + [other[1]], itab, stab, sem)
    safe = places(blocks[0][0]) // tj
    for q in range(n):
        base = (me ^ q) * rows

        def strip(i, done, q=q, base=base, low=False):
            tiles = [whole_tile(blocks[q], stab[q, i * tj + j], low) for j in range(tj)]
            panel_ref[pl.ds(pl.multiple_of(base + i * TB, TB), TB), :] = jnp.concatenate(tiles, axis=1)
            return done

        lax.fori_loop(0, safe, functools.partial(strip, low=True), 0, unroll=2)
        lax.fori_loop(safe, ti, strip, 0, unroll=2)
    mine = blocks[0]
    heads_rests = (mine[0], other[0], mine[1], other[1])
    products("whole", heads_rests, 0, panel_ref, stab, (0, n), lhs, rows, adder(acc_ref, None, rows))


def panel(payloads, other, rows, cols):
    n = len(payloads)
    return pl.pallas_call(
        functools.partial(panel_kernel, n, rows),
        out_shape=(
            jax.ShapeDtypeStruct((n * rows, cols), BF16),
            jax.ShapeDtypeStruct((rows, cols), F32),
        ),
        in_specs=[VMEM] * (2 * n + 2),
        out_specs=(VMEM, VMEM),
        scratch_shapes=dot_scratch(n + 1, rows, cols),
        compiler_params=params(24),
        cost_estimate=cost(4 * rows * cols * cols, 2 * n * rows * cols * 2),
        name="panel",
    )(*[x for p in payloads for x in p], *other)


def dot_kernel(kind, pairs, rows, *refs):
    blocks = regroup(refs, [4] * len(pairs))
    panel_ref, prior_ref, acc_ref, itab, stab, sem, lhs = refs[4 * len(pairs) :]
    read_tables([r for b in blocks for r in b[:2]], itab, stab, sem)
    for k, (pair, b) in enumerate(zip(pairs, blocks)):
        use = adder(acc_ref, acc_ref if k else prior_ref, rows)
        products(kind, b, pair, panel_ref, stab, (2 * k, 2 * k + 1), lhs, rows, use)


def head_kernel(side, pair, rows, head_ref, panel_ref, prior_ref, acc_ref, itab, stab, sem, lhs):
    read_tables([head_ref], itab, stab, sem)
    use = adder(acc_ref, prior_ref, rows)
    products("heads", [head_ref], pair, panel_ref, stab, (0,), lhs, rows, use, sides=(side,))


def add_products(kernel, payloads, dense, prior, rows, n_tables):
    cols = dense.shape[1]
    return pl.pallas_call(
        kernel,
        out_shape=jax.ShapeDtypeStruct((rows, cols), F32),
        in_specs=[VMEM] * (len(payloads) + 2),
        out_specs=VMEM,
        scratch_shapes=dot_scratch(n_tables, rows, cols),
        input_output_aliases={len(payloads) + 1: 0},
        compiler_params=params(24),
        cost_estimate=cost(2 * rows * cols * cols * n_tables, 12 * rows * cols),
        name="dots",
    )(*payloads, dense, prior)


def dots(blocks, pairs, dense, prior, rows):
    kernel = functools.partial(dot_kernel, "all", pairs, rows)
    return add_products(kernel, [x for b in blocks for x in b], dense, prior, rows, 2 * len(pairs))


def head_dots(head, side, pair, dense, prior, rows):
    kernel = functools.partial(head_kernel, side, pair, rows)
    return add_products(kernel, [head], dense, prior, rows, 1)


def total_kernel(*refs):
    refs[-1][...] = functools.reduce(jnp.add, [r[...] for r in refs[:-1]])


def total_of(xs):
    return pl.pallas_call(
        total_kernel,
        out_shape=jax.ShapeDtypeStruct(xs[0].shape, F32),
        in_specs=[VMEM] * len(xs),
        out_specs=VMEM,
        compiler_params=params(4),
        cost_estimate=cost(1e5, 4 * xs[0].size * len(xs)),
        name="total",
    )(*xs)


def means_kernel(n_pairs, s_rows, order, *refs):
    msgs, (thr_ref, panel_ref, out_ref, flag_ref) = refs[:n_pairs], refs[n_pairs:]
    _, z, core = place()
    cols = panel_ref.shape[1]
    tj = cols // TB
    total = jnp.zeros((8, cols), F32)
    row = lax.broadcasted_iota(I32, (8, TB), 0)
    over = jnp.zeros((1, TB), F32)
    for q in range(n_pairs):
        for b in range(2):
            over = jnp.maximum(over, msgs[q][b * s_rows + tj : b * s_rows + tj + 1, :])
            for t in range(tj):
                s = jnp.broadcast_to(msgs[q][b * s_rows + t : b * s_rows + t + 1, :], (8, TB))
                high = s.astype(BF16).astype(F32)
                mid = (s - high).astype(BF16).astype(F32)
                low = s - high - mid
                lhs = jnp.where(row == 0, high, jnp.where(row == 1, mid, jnp.where(row == 2, low, 0.0)))
                at = (z ^ q) * 2 * cols + (core ^ b) * cols + t * TB
                total += jnp.dot(
                    lhs.astype(BF16),
                    panel_ref[pl.ds(pl.multiple_of(at, TB), TB), :],
                    preferred_element_type=F32,
                )
    mean = jnp.sum(total, axis=0, keepdims=True) / order
    out_ref[...] = jnp.broadcast_to(0.125 * thr_ref[...].astype(F32) * mean, out_ref.shape)
    flag_ref[0] = jnp.where(jnp.max(over) > 0.0, 1, 0).astype(I32)


def cuts_of(messages, thr, dense, s_rows, order):
    n = len(messages)
    cols = dense.shape[1]
    return pl.pallas_call(
        functools.partial(means_kernel, n, s_rows, order),
        out_shape=(jax.ShapeDtypeStruct((8, cols), F32), jax.ShapeDtypeStruct((1,), I32)),
        in_specs=[VMEM] * (n + 2),
        out_specs=(VMEM, SMEM),
        compiler_params=params(12),
        cost_estimate=cost(1e7, dense.size * 2),
        name="cuts",
    )(*messages, thr, dense)


def last_kernel(pair, rows, *refs):
    blocks, (panel_ref, prior_ref, cut_ref, keep_ref, acc_ref, tot_ref) = refs[:4], refs[4:10]
    itab, stab, sem, lhs = refs[10:]
    step = strip_rows(rows)
    cols = panel_ref.shape[1]
    per = step // TB
    totals = [jnp.zeros((8, cols), F32)]
    tables = start_tables(blocks[:2], itab, stab, sem)

    def use(m, got):
        prior = prior_ref[m * step : (m + 1) * step, :]
        got = jnp.maximum((prior if got is None else prior + got) - cut_ref[0:1, :], 0.0)
        for a in range(per):
            i = m * per + a
            cell = got[a * TB : (a + 1) * TB, :] * keep_ref[i : i + 1, :]
            acc_ref[i * TB : (i + 1) * TB, :] = cell
            totals[0] += jnp.sum(cell.reshape(TB // 8, 8, cols), axis=0)

    products("pools", blocks, pair, panel_ref, stab, (0, 1), lhs, rows, use, tables=tables)
    tot_ref[...] = jnp.sum(totals[0], axis=0, keepdims=True)


def finish(keep, blocks, pair, dense, prior, cut, rows):
    cols = dense.shape[1]
    return pl.pallas_call(
        functools.partial(last_kernel, pair, rows),
        out_shape=(jax.ShapeDtypeStruct((rows, cols), F32), jax.ShapeDtypeStruct((1, cols), F32)),
        in_specs=[VMEM] * 8,
        out_specs=(VMEM, VMEM),
        scratch_shapes=dot_scratch(2, rows, cols),
        compiler_params=params(20),
        cost_estimate=cost(4 * rows * cols * cols, 12 * rows * cols),
        name="finish",
    )(*blocks, dense, prior, cut, keep)


def scale_kernel(n, order, x_ref, *refs):
    tots, out_ref = refs[:n], refs[n]
    total = tots[0][...]
    for t in tots[1:]:
        total = total + t[...]
    total = total / order
    factor = 1.0 / jnp.maximum(total, 0.1)
    out_ref[...] = (x_ref[...] * factor).astype(BF16)


def scale(x, totals, order):
    n = len(totals)
    return pl.pallas_call(
        functools.partial(scale_kernel, n, order),
        out_shape=jax.ShapeDtypeStruct(x.shape, BF16),
        in_specs=[VMEM] * (n + 1),
        out_specs=VMEM,
        compiler_params=params(12),
        cost_estimate=cost(2 * x.size, 6 * x.size),
        name="scale",
    )(x, *totals)


def dense_path(values, tile_mask, keep_mask, thr_index, n_row, n_col):
    rows, cols = values.shape
    ti, tj = tiles_of(values.shape)
    matrix = (
        values.reshape(ti, TB, tj, TB) * tile_mask[:, None, :, None].astype(BF16)
    ).reshape(rows, cols)
    kept = jnp.broadcast_to(keep_mask[:, None, :, None].astype(F32), (ti, TB, tj, TB)).reshape(rows, cols)
    r, c = lax.axis_index("row"), lax.axis_index("col")
    order = rows * n_row

    def col_ring(i, carry):
        block, panel_ = carry
        panel_ = lax.dynamic_update_slice(panel_, block, (((r - i) % n_row) * rows, 0))
        return lax.ppermute(block, "row", [(k, (k + 1) % n_row) for k in range(n_row)]), panel_

    _, panel_ = lax.fori_loop(0, n_row, col_ring, (matrix, jnp.zeros((order, cols), BF16)))

    def row_ring(i, carry):
        block, acc = carry
        part = lax.dynamic_slice(panel_, (((c - i) % n_col) * cols, 0), (cols, cols))
        acc = acc + jnp.dot(block, part, preferred_element_type=F32)
        return lax.ppermute(block, "col", [(k, (k + 1) % n_col) for k in range(n_col)]), acc

    _, product = lax.fori_loop(0, n_col, row_ring, (matrix, jnp.zeros((rows, cols), F32)))
    means = lax.psum(jnp.sum(product, axis=0), "row") / order
    pruned = jnp.maximum(product - 0.125 * thr_index.astype(F32) * means, 0.0) * kept
    totals = lax.psum(jnp.sum(pruned, axis=0), "row") / order
    return (pruned / jnp.maximum(totals, 0.1)).astype(BF16)


def on_device(values, tile_mask, keep_mask, thr_index, n_row, n_col):
    return body(values, tile_mask, keep_mask, thr_index, n_row, n_col)


def body(values, tile_mask, keep_mask, thr_index, n_row, n_col):
    rows, cols = values.shape
    ti, tj = tiles_of(values.shape)
    first = ti * tj // 2
    extra = ti * tj * 3 // 16
    slots = ti * tj * 13 // 16
    n_z = n_col // 2
    last = n_z - 1
    order = rows * n_row

    def send(x, dr=0, dz=0, dc=0):
        pairs = [
            (r * n_col + z * 2 + c, (r ^ dr) * n_col + (z ^ dz) * 2 + (c ^ dc))
            for r in range(n_row)
            for z in range(n_z)
            for c in range(2)
        ]
        return lax.ppermute(x, AXES, pairs)

    own = pack(values, tile_mask.T, slots, first)
    own_swapped = [send(x, dc=1) for x in own]
    spare, sums = pool(values, tile_mask.T, own[1], own_swapped[1], first, extra)

    line = {0: [own[0], spare]}
    swapped = {}
    for j in range(1, n_z):
        low = j & -j
        line[j] = [send(x, dz=low) for x in line[j ^ low]]
        swapped[j] = [send(x, dc=1) for x in line[j]]

    column = {0: own}
    for q in range(1, n_row):
        low = q & -q
        rest = q ^ low
        if rest and rest & -rest == rest:
            column[q] = [send(column[low][0], dr=rest), send(column[rest][1], dr=low)]
        else:
            column[q] = [send(x, dr=q) for x in own]

    dense, acc = panel([column[q] for q in range(n_row)], own_swapped, rows, cols)

    sums = [sums] + [send(sums, dr=q) for q in range(1, n_row)]
    sums = total_of(sums)
    both = jnp.concatenate([sums, send(sums, dc=1)], axis=0)
    messages = [both] + [send(both, dz=j) for j in range(1, n_z)]
    cut, over = cuts_of(messages, thr_index.reshape(1, cols), dense, sums.shape[0], order)

    early = tuple(range(1, last))
    if early:
        blocks = [(line[j][0], swapped[j][0], line[j][1], swapped[j][1]) for j in early]
        acc = dots(blocks, early, dense, acc, rows)
    acc = head_dots(line[last][0], 0, last, dense, acc, rows)
    acc = head_dots(swapped[last][0], 1, last, dense, acc, rows)
    keep = jnp.repeat(keep_mask.astype(F32), TB, axis=1)

    def fast():
        blocks = (line[last][0], swapped[last][0], line[last][1], swapped[last][1])
        pruned, tot = finish(keep, blocks, last, dense, acc, cut, rows)
        bit = n_row // 2
        while bit:
            tot = tot + send(tot, dr=bit)
            bit //= 2
        return scale(pruned, [tot], order)

    def full():
        return dense_path(values, tile_mask, keep_mask, thr_index, n_row, n_col)

    return lax.cond(over[0] > 0, full, fast)


def solution(mesh):
    n_row, n_col = mesh.shape["row"], mesh.shape["col"]
    return jax.shard_map(
        functools.partial(on_device, n_row=n_row, n_col=n_col),
        mesh=mesh,
        in_specs=(P("row", "col"), P("row", "col"), P("row", "col"), P("col")),
        out_specs=P("row", "col"),
        check_vma=False,
    )
```
